32 devices in a mesh: rep: 2 (over x), frame: 4 (over z), tensor: 4 (over y, core).
Axes of the slice: x: 2, y: 2, z: 4, core: 2. Of those that a mesh axis runs over, the one named last changes fastest.
Arguments:
- tokens: bfloat16 [4, 16, 196, 768], P('rep', 'frame', 'tensor'), may hold values from -6 to 6
- query_space: bfloat16 [768, 768], P('frame', 'tensor'), may hold values from -0.3125 to 0.3125
- key_space: bfloat16 [768, 768], P('frame', 'tensor'), may hold values from -0.3125 to 0.3125
- value_space: bfloat16 [768, 768], P('frame', 'tensor'), may hold values from -0.21875 to 0.21875
- output_space: bfloat16 [768, 768], P('tensor', 'frame'), may hold values from -0.625 to 0.625
- query_time: bfloat16 [768, 768], P('frame', 'tensor'), may hold values from -0.3125 to 0.3125
- key_time: bfloat16 [768, 768], P('frame', 'tensor'), may hold values from -0.3125 to 0.3125
- value_time: bfloat16 [768, 768], P('frame', 'tensor'), may hold values from -0.21875 to 0.21875
- output_time: bfloat16 [768, 768], P('tensor', 'frame'), may hold values from -0.4375 to 0.4375
- mlp_in: bfloat16 [768, 3072], P('frame', 'tensor'), may hold values from -0.21875 to 0.21875
- bias_in: bfloat16 [3072], P('tensor'), may hold values from -3 to 3
- mlp_out: bfloat16 [3072, 768], P('tensor', 'frame'), may hold values from -0.109375 to 0.109375
- bias_out: bfloat16 [768], P('frame'), may hold values from -2 to 2
- gain_first: float32 [768], P(('frame', 'tensor')), may hold values from 0.5 to 1.5
- shift_first: float32 [768], P(('frame', 'tensor')), may hold values from -2 to 2
- gain_second: float32 [768], P(('frame', 'tensor')), may hold values from 0.5 to 1.5
- shift_second: float32 [768], P(('frame', 'tensor')), may hold values from -2 to 2
- gain_third: float32 [768], P(('frame', 'tensor')), may hold values from 0.5 to 1.5
- shift_third: float32 [768], P(('frame', 'tensor')), may hold values from -2 to 2
- place_slot: int32 [196], replicated, may hold values from -1 to 255, as said below
- cotangent: bfloat16 [4, 16, 196, 768], P('rep', 'frame', 'tensor'), may hold values from -6 to 6
Outputs:
- result: bfloat16 [4, 16, 196, 768], P('rep', 'frame', 'tensor')
- grad_tokens: float32 [4, 16, 196, 768], P('rep', 'frame', 'tensor')
- grad_query_space: float32 [768, 768], P('frame', 'tensor')
- grad_key_space: float32 [768, 768], P('frame', 'tensor')
- grad_value_space: float32 [768, 768], P('frame', 'tensor')
- grad_output_space: float32 [768, 768], P('tensor', 'frame')
- grad_query_time: float32 [768, 768], P('frame', 'tensor')
- grad_key_time: float32 [768, 768], P('frame', 'tensor')
- grad_value_time: float32 [768, 768], P('frame', 'tensor')
- grad_output_time: float32 [768, 768], P('tensor', 'frame')
- grad_mlp_in: float32 [768, 3072], P('frame', 'tensor')
- grad_bias_in: float32 [3072], P('tensor')
- grad_mlp_out: float32 [3072, 768], P('tensor', 'frame')
- grad_bias_out: float32 [768], P('frame')
- grad_gain_first: float32 [768], P(('frame', 'tensor'))
- grad_shift_first: float32 [768], P(('frame', 'tensor'))
- grad_gain_second: float32 [768], P(('frame', 'tensor'))
- grad_shift_second: float32 [768], P(('frame', 'tensor'))
- grad_gain_third: float32 [768], P(('frame', 'tensor'))
- grad_shift_third: float32 [768], P(('frame', 'tensor'))
The draws below stay inside these ranges and needn't reach their ends.
Inputs may be any that keep to these rules, and one draw needn't show every extreme that they name: `place_slot`: each unmasked place has a slot of its own; a slot s is taken by frame index s // 64; exactly 64 places have slots of one frame index; at least 64 places are unmasked; slot 255 is always taken; a masked place is masked in every frame of every clip.
All inputs are finite; a program needn't handle non-finite values.
Results may differ from the reference program's by a relative error of at most 0.023.
Values may be sent and summed in bfloat16 or wider, within the bound.
A program may use at most 192 MiB of HBM per device.

```python
from functools import partial
import jax
import jax.numpy as jnp
from jax import lax

D = 768
HEADS = 12
HEAD_DIM = 64
FF = 3072
FRAMES = 16
PLACES = 196
CAP = 64
CLIPS = 4
SLOTS = 256


def draw_place_slot(key, part):
    key_order = jax.random.fold_in(key, 11)
    key_pick = jax.random.fold_in(key, 12)
    key_device = jax.random.fold_in(key, 13)
    ranking = jax.random.permutation(key_order, PLACES).astype(jnp.int32)
    devices = SLOTS // CAP
    full_device = jax.random.randint(key_device, (), 0, devices).astype(jnp.int32)
    others = SLOTS - CAP
    pool_size = others + PLACES // 4 + 1
    rest = jax.random.permutation(key_pick, pool_size - 1).astype(jnp.int32)
    rest = rest + (rest >= others - 1).astype(jnp.int32)
    pick_order = jnp.concatenate((jnp.full((1,), others - 1, jnp.int32), rest)).astype(jnp.int32)
    later_rank = jnp.maximum(ranking - CAP, 0)
    chosen = pick_order[later_rank]
    mapped = chosen + CAP * (chosen >= full_device * CAP).astype(jnp.int32)
    spread_slot = jnp.where(chosen >= others, -1, mapped)
    return jnp.where(ranking < CAP, full_device * CAP + ranking, spread_slot).astype(jnp.int32)


def steps_of(stream_key, extent, split, smallest, largest):
    def one(dim, parts):
        heights = jax.random.uniform(jax.random.fold_in(jax.random.fold_in(stream_key, 6), dim), (parts,), jnp.float32, smallest / len(split), largest / len(split))
        return jnp.repeat(jnp.exp(heights), extent[dim] // parts).reshape((-1,) + (1,) * (len(extent) - dim - 1))

    gain = one(*split[0])
    for cut in split[1:]:
        gain = gain * one(*cut)
    return gain


def bell_draw(key, extent, scale, reach, shards=(), kind=jnp.bfloat16):
    result = scale * jax.random.normal(key, extent, jnp.float32)
    if shards:
        result = result * steps_of(key, extent, shards, -0.22, 0.18)
    return jnp.clip(result, -reach, reach).astype(kind)


def setup_inputs(seed: int = 0) -> dict:
    seeds = jax.random.split(jax.random.key(seed), 22)
    tokens = bell_draw(seeds[0], (CLIPS, FRAMES, PLACES, D), 1.0, 6.0, ((0, 2), (1, 4), (2, 4)))
    query_space = bell_draw(seeds[1], (D, D), (D // 2) ** -0.5, 0.3125, ((0, 4), (1, 4)))
    key_space = bell_draw(seeds[2], (D, D), (D // 2) ** -0.5, 0.3125, ((0, 4), (1, 4)))
    value_space = bell_draw(seeds[3], (D, D), D ** -0.5, 0.21875, ((0, 4), (1, 4)))
    output_space = bell_draw(seeds[4], (D, D), (D // 8) ** -0.5, 0.625, ((0, 4), (1, 4)))
    query_time = bell_draw(seeds[5], (D, D), (D // 2) ** -0.5, 0.3125, ((0, 4), (1, 4)))
    key_time = bell_draw(seeds[6], (D, D), (D // 2) ** -0.5, 0.3125, ((0, 4), (1, 4)))
    value_time = bell_draw(seeds[7], (D, D), D ** -0.5, 0.21875, ((0, 4), (1, 4)))
    output_time = bell_draw(seeds[8], (D, D), (D // 4) ** -0.5, 0.4375, ((0, 4), (1, 4)))
    mlp_in = bell_draw(seeds[9], (D, FF), D ** -0.5, 0.21875, ((0, 4), (1, 4)))
    bias_in = bell_draw(seeds[10], (FF,), 0.5, 3.0, ((0, 4),))
    mlp_out = bell_draw(seeds[11], (FF, D), FF ** -0.5, 0.109375, ((0, 4), (1, 4)))
    bias_out = bell_draw(seeds[12], (D,), 0.3, 2.0, ((0, 4),))
    gain_first = jnp.clip(1.0 + 0.1 * jax.random.normal(seeds[13], (D,), jnp.float32), 0.5, 1.5)
    shift_first = bell_draw(seeds[14], (D,), 0.3, 2.0, ((0, 16),), jnp.float32)
    gain_second = jnp.clip(1.0 + 0.1 * jax.random.normal(seeds[15], (D,), jnp.float32), 0.5, 1.5)
    shift_second = bell_draw(seeds[16], (D,), 0.3, 2.0, ((0, 16),), jnp.float32)
    gain_third = jnp.clip(1.0 + 0.1 * jax.random.normal(seeds[17], (D,), jnp.float32), 0.5, 1.5)
    shift_third = bell_draw(seeds[18], (D,), 0.3, 2.0, ((0, 16),), jnp.float32)
    place_slot = draw_place_slot(jax.random.fold_in(seeds[21], 71), 0)
    cotangent = bell_draw(seeds[20], (CLIPS, FRAMES, PLACES, D), 1.0, 6.0, ((0, 2), (1, 4), (2, 4)))
    return {"tokens": tokens, "query_space": query_space, "key_space": key_space, "value_space": value_space, "output_space": output_space, "query_time": query_time, "key_time": key_time, "value_time": value_time, "output_time": output_time, "mlp_in": mlp_in, "bias_in": bias_in, "mlp_out": mlp_out, "bias_out": bias_out, "gain_first": gain_first, "shift_first": shift_first, "gain_second": gain_second, "shift_second": shift_second, "gain_third": gain_third, "shift_third": shift_third, "place_slot": place_slot, "cotangent": cotangent}


@jax.custom_vjp
def low(v):
    return lax.optimization_barrier(v.astype(jnp.bfloat16)).astype(jnp.float32)

@jax.custom_vjp
def low_back(v):
    return v

def low_keep(v):
    return (low(v), None)

def low_pass(kept, grad):
    return (grad,)

def back_keep(v):
    return (v, None)

def back_low(kept, grad):
    return (low(grad),)
low.defvjp(low_keep, low_pass)
low_back.defvjp(back_keep, back_low)
precise = lax.Precision.HIGHEST

def norm_rows(values, gain_vec, shift_vec):
    centre = lax.optimization_barrier(jnp.mean(values, axis=-1, keepdims=True))
    offset = values - centre
    spread = lax.optimization_barrier(jnp.mean(offset * offset, axis=-1, keepdims=True))
    return offset * lax.rsqrt(spread + 1e-06) * gain_vec + shift_vec

def project(values, matrix):
    return jnp.einsum('fpd,dk->fpk', values, matrix, precision=precise)

def heads_of(values, matrix):
    frame_count, place_count = (values.shape[0], values.shape[1])
    return low(low_back(project(values, matrix))).reshape(frame_count, place_count, HEADS, HEAD_DIM)

def space_branch(normed, query_w, key_w, value_w, output_w, key_bias):
    frame_count, place_count = (normed.shape[0], normed.shape[1])
    queries = heads_of(normed, query_w)
    key_rows = heads_of(normed, key_w)
    value_rows = heads_of(normed, value_w)
    scores = jnp.einsum('fphe,fqhe->fhpq', queries, key_rows, precision=precise) * HEAD_DIM ** (-0.5)
    scores = low_back(scores + key_bias[None, None, None, :])
    attn_probs = low(jax.nn.softmax(scores, axis=-1))
    attended = jnp.einsum('fhpq,fqhe->fphe', attn_probs, value_rows, precision=precise)
    attended = low(low_back(attended.reshape(frame_count, place_count, D)))
    return low_back(project(attended, output_w))

def time_branch(normed, query_w, key_w, value_w, output_w, keep_mask):
    frame_count, place_count = (normed.shape[0], normed.shape[1])
    queries = heads_of(normed, query_w)
    key_rows = heads_of(normed, key_w)
    value_rows = heads_of(normed, value_w)
    scores = jnp.einsum('fphe,gphe->phfg', queries, key_rows, precision=precise) * HEAD_DIM ** (-0.5)
    scores = low_back(scores)
    attn_probs = low(jax.nn.softmax(scores, axis=-1))
    attended = jnp.einsum('phfg,gphe->fphe', attn_probs, value_rows, precision=precise)
    attended = attended * keep_mask[None, :, None, None]
    attended = low(low_back(attended.reshape(frame_count, place_count, D)))
    return low_back(project(attended, output_w))

def mlp_branch(normed, weight_in, bias_vec_in, weight_out, bias_vec_out):
    before = low_back(project(normed, weight_in) + bias_vec_in)
    hidden = low(jax.nn.gelu(before, approximate=True))
    return low_back(project(hidden, weight_out) + bias_vec_out)

def layer(values, weights, keep_mask, key_bias):
    query_space, key_space, value_space, output_space, query_time, key_time, value_time, output_time, mlp_in, bias_in, mlp_out, bias_out, gain_first, shift_first, gain_second, shift_second, gain_third, shift_third = weights
    after_space = values + space_branch(low(norm_rows(values, gain_first, shift_first)), query_space, key_space, value_space, output_space, key_bias)
    after_time = after_space + time_branch(low(norm_rows(after_space, gain_second, shift_second)), query_time, key_time, value_time, output_time, keep_mask)
    return after_time + mlp_branch(low(norm_rows(after_time, gain_third, shift_third)), mlp_in, bias_in, mlp_out, bias_out)

def reference(tokens, query_space, key_space, value_space, output_space, query_time, key_time, value_time, output_time, mlp_in, bias_in, mlp_out, bias_out, gain_first, shift_first, gain_second, shift_second, gain_third, shift_third, place_slot, cotangent):
    params = tuple((weight.astype(jnp.float32) for weight in (query_space, key_space, value_space, output_space, query_time, key_time, value_time, output_time, mlp_in, bias_in, mlp_out, bias_out, gain_first, shift_first, gain_second, shift_second, gain_third, shift_third)))
    keep_mask = (place_slot >= 0).astype(jnp.float32)
    key_bias = jnp.where(place_slot >= 0, 0.0, -1e+30).astype(jnp.float32)

    def step(totals, clip):
        clip_in, clip_cot = clip
        layer_fn = partial(layer, keep_mask=keep_mask, key_bias=key_bias)
        outputs, pullback = jax.vjp(layer_fn, clip_in.astype(jnp.float32), params)
        grad_in, grad_weights = pullback(clip_cot.astype(jnp.float32))
        totals = tuple((total + grad for total, grad in zip(totals, grad_weights)))
        return (totals, (outputs.astype(jnp.bfloat16), grad_in))
    zeros = tuple((jnp.zeros_like(weight) for weight in params))
    totals, (outputs, grads_in) = lax.scan(step, zeros, (tokens, cotangent))
    return (outputs, grads_in, totals[0], totals[1], totals[2], totals[3], totals[4], totals[5], totals[6], totals[7], totals[8], totals[9], totals[10], totals[11], totals[12], totals[13], totals[14], totals[15], totals[16], totals[17])
```

```python
from functools import partial

import jax
import jax.numpy as jnp
from jax import lax
from jax.experimental import pallas as pl
from jax.experimental.pallas import tpu as pltpu
from jax.sharding import PartitionSpec as P

HEAD = 64
PAD = 56
BF = jnp.bfloat16
F32 = jnp.float32
NT = (((1,), (1,)), ((), ()))
TN = (((0,), (0,)), ((), ()))
GELU_C = 0.7978845608028654
SCALE = HEAD ** (-0.5)


def dot(a, b, dims=(((1,), (0,)), ((), ()))):
    return lax.dot_general(a, b, dims, preferred_element_type=F32)


def norm_stats(v):
    m = jnp.mean(v, axis=-1, keepdims=True)
    off = v - m
    s = jnp.mean(off * off, axis=-1, keepdims=True)
    r = lax.rsqrt(s + 1e-06)
    return off * r, r


def norm(v, g, b):
    xhat, _ = norm_stats(v)
    return xhat * g + b


def norm_back(v, g, dy):
    xhat, r = norm_stats(v)
    dyg = dy * g
    mean1 = jnp.mean(dyg, axis=-1, keepdims=True)
    mean2 = jnp.mean(dyg * xhat, axis=-1, keepdims=True)
    dx = r * (dyg - mean1 - xhat * mean2)
    dgain = jnp.sum(dy * xhat, axis=0, keepdims=True)
    dshift = jnp.sum(dy, axis=0, keepdims=True)
    return dx, dgain, dshift


def softmax(s):
    m = jnp.max(s, axis=-1, keepdims=True)
    e = jnp.exp(s - m)
    return e / jnp.sum(e, axis=-1, keepdims=True)


def attend_head(q, k, v, bias):
    s = dot(q, k, NT) * SCALE + bias
    p = softmax(s)
    return dot(p.astype(BF), v).astype(BF)


def attend_head_back(do, q, k, v, bias):
    s = dot(q, k, NT) * SCALE + bias
    p = softmax(s)
    dp = dot(do, v, NT)
    dv = dot(p.astype(BF), do, TN)
    inner = jnp.sum(dp * p, axis=-1, keepdims=True)
    ds = (p * (dp - inner)).astype(BF)
    dq = dot(ds, k) * SCALE
    dk = dot(ds, q, TN) * SCALE
    return dq.astype(BF), dk.astype(BF), dv.astype(BF)


def space_forward(width, heads, frames, rows, x_ref, vec_ref, bias_ref, w_ref, qkv_ref, os_ref, xs_ref, ht_ref, h_scr):
    t = pl.program_id(0)

    @pl.when(t == 0)
    def _():
        x = x_ref[...].astype(F32)
        h_scr[...] = norm(x, vec_ref[0:1, :], vec_ref[1:2, :]).astype(BF)
        xs_ref[...] = x

    qkv_ref[0] = dot(h_scr[...], w_ref[0, 0, :, : 3 * width]).astype(BF)
    bias = bias_ref[...]
    for i in range(frames):
        r = pl.ds(i * rows, rows)
        for h in range(heads):
            q = qkv_ref[0, r, h * HEAD : (h + 1) * HEAD]
            k = qkv_ref[0, r, width + h * HEAD : width + (h + 1) * HEAD]
            v = qkv_ref[0, r, 2 * width + h * HEAD : 2 * width + (h + 1) * HEAD]
            os_ref[0, r, h * HEAD : (h + 1) * HEAD] = attend_head(q, k, v, bias)
    xs_ref[...] += dot(os_ref[0], w_ref[0, 0, :, 3 * width :], NT)

    @pl.when(t == pl.num_programs(0) - 1)
    def _():
        ht_ref[...] = norm(xs_ref[...], vec_ref[2:3, :], vec_ref[3:4, :]).astype(BF)


def space_backward(
    width, heads, frames, rows,
    x_ref, xs_ref, gt_ref, dht_ref, vec_ref, bias_ref, w_ref, qkv_ref, os_ref,
    gx_ref, gw_ref, sv_ref, h_scr, gs_scr, dat_scr, dh_scr, dqkv_scr,
):
    t = pl.program_id(0)

    @pl.when(t == 0)
    def _():
        x = x_ref[...].astype(F32)
        h_scr[...] = norm(x, vec_ref[0:1, :], vec_ref[1:2, :]).astype(BF)
        dx, dg, db = norm_back(xs_ref[...], vec_ref[2:3, :], dht_ref[...].astype(F32))
        gs = gt_ref[...] + dx
        gs_scr[...] = gs
        dat_scr[...] = gs.astype(BF)
        sv_ref[2:3, :] = dg
        sv_ref[3:4, :] = db
        sv_ref[4:8, :] = jnp.zeros((4, sv_ref.shape[1]), F32)
        dh_scr[...] = jnp.zeros_like(dh_scr)

    dat = dat_scr[...]
    dos = dot(dat, w_ref[0, 0, :, 3 * width :]).astype(BF)
    bias = bias_ref[...]
    for i in range(frames):
        r = pl.ds(i * rows, rows)
        for h in range(heads):
            a, b, c = (slice(j * width + h * HEAD, j * width + (h + 1) * HEAD) for j in range(3))
            dq, dk, dv = attend_head_back(
                dos[i * rows : (i + 1) * rows, a], qkv_ref[0, r, a], qkv_ref[0, r, b], qkv_ref[0, r, c], bias
            )
            dqkv_scr[r, a] = dq
            dqkv_scr[r, b] = dk
            dqkv_scr[r, c] = dv
    dqkv = dqkv_scr[...]
    gw_ref[0, :, : 3 * width] = dot(h_scr[...], dqkv, TN).astype(BF)
    gw_ref[0, :, 3 * width :] = dot(dat, os_ref[0], TN).astype(BF)
    dh_scr[...] += dot(dqkv, w_ref[0, 0, :, : 3 * width], NT)

    @pl.when(t == pl.num_programs(0) - 1)
    def _():
        dx, dg, db = norm_back(x_ref[...].astype(F32), vec_ref[0:1, :], dh_scr[...])
        gx_ref[...] = (gs_scr[...] + dx).astype(gx_ref.dtype)
        sv_ref[0:1, :] = dg
        sv_ref[1:2, :] = db


def group_bias(size, places):
    i = lax.broadcasted_iota(jnp.int32, (size, size), 0)
    j = lax.broadcasted_iota(jnp.int32, (size, size), 1)
    return jnp.where(i % places == j % places, 0.0, -1e30).astype(F32)


def time_forward(width, heads, groups, size, places, core_ref, h_ref, w_ref, mask_ref, qkv_ref, ot_ref):
    qkv_ref[0] = dot(h_ref[...], w_ref[0, 0, :, : 3 * width]).astype(BF)
    bias = group_bias(size, places)

    def one(g, carry):
        r = pl.ds(pl.multiple_of(g * size, size), size)
        keep = mask_ref[r, :]
        for h in range(heads):
            a, b, c = (slice(j * width + h * HEAD, j * width + (h + 1) * HEAD) for j in range(3))
            s = dot(qkv_ref[0, r, a], qkv_ref[0, r, b], NT) * SCALE + bias
            o = dot(softmax(s).astype(BF), qkv_ref[0, r, c])
            ot_ref[0, r, a] = jnp.where(keep > 0, o, 0.0).astype(BF)
        return carry

    lax.fori_loop(0, groups, one, 0)


def time_backward(
    width, heads, groups, size, places, core_ref, h_ref, w_ref, mask_ref, qkv_ref, do_ref, gw_ref, dh_ref, dqkv_scr
):
    bias = group_bias(size, places)

    def one(g, carry):
        r = pl.ds(pl.multiple_of(g * size, size), size)
        keep = mask_ref[r, :]
        for h in range(heads):
            a, b, c = (slice(j * width + h * HEAD, j * width + (h + 1) * HEAD) for j in range(3))
            do = jnp.where(keep > 0, do_ref[0, r, a].astype(F32), 0.0).astype(BF)
            dq, dk, dv = attend_head_back(do, qkv_ref[0, r, a], qkv_ref[0, r, b], qkv_ref[0, r, c], bias)
            dqkv_scr[r, a] = dq
            dqkv_scr[r, b] = dk
            dqkv_scr[r, c] = dv
        return carry

    lax.fori_loop(0, groups, one, 0)
    dqkv = dqkv_scr[...]
    gw_ref[0] = dot(h_ref[...], dqkv, TN).astype(BF)
    dh = dot(dqkv, w_ref[0, 0, :, : 3 * width], NT)

    @pl.when(pl.program_id(0) == 0)
    def _():
        dh_ref[...] = dh

    @pl.when(pl.program_id(0) > 0)
    def _():
        dh_ref[...] += dh


def mlp_both(
    width, tensors,
    xs_ref, cot_ref, ot_ref, vec_ref, bin_ref, wt_ref, win_ref, wout_ref,
    res_ref, gt_ref, do_ref, gin_ref, gout_ref, gwt_ref, sv_ref, gb_ref,
    xt_scr, hm_scr, xm_scr, dhm_scr,
):
    t = pl.program_id(0)

    @pl.when(t == 0)
    def _():
        xt = xs_ref[...]
        for j in range(tensors):
            xt = xt + dot(ot_ref[j], wt_ref[0, j, :, 3 * width :], NT)
        xt_scr[...] = xt
        hm_scr[...] = norm(xt, vec_ref[4:5, :], vec_ref[5:6, :]).astype(BF)
        xm_scr[...] = xt + vec_ref[6:7, :]
        dhm_scr[...] = jnp.zeros_like(dhm_scr)

    hm = hm_scr[...]
    dz = cot_ref[...]
    win = win_ref[0, 0]
    wout = wout_ref[0, 0]
    pre = dot(hm, win) + bin_ref[pl.ds(t, 1), :]
    sq = pre * pre
    th = jnp.tanh(GELU_C * (pre + 0.044715 * (pre * sq)))
    hidden = (0.5 * pre * (1.0 + th)).astype(BF)
    xm_scr[...] += dot(hidden, wout, NT)
    slope = 0.5 * (1.0 + th) + 0.5 * pre * (1.0 - th * th) * (GELU_C * (1.0 + 0.134145 * sq))
    dpre = dot(dz, wout) * slope
    dpre_b = dpre.astype(BF)
    gb_ref[pl.ds(t, 1), :] = jnp.sum(dpre_b.astype(F32), axis=0, keepdims=True)
    gout_ref[0] = dot(dz, hidden, TN).astype(BF)
    gin_ref[0] = dot(hm, dpre_b, TN).astype(BF)
    dhm_scr[...] += dot(dpre_b, win, NT)

    @pl.when(t == pl.num_programs(0) - 1)
    def _():
        res_ref[...] = xm_scr[...].astype(BF)
        gm = dz.astype(F32)
        dx, dg, db = norm_back(xt_scr[...], vec_ref[4:5, :], dhm_scr[...])
        gt = gm + dx
        gt_ref[...] = gt
        dat = gt.astype(BF)
        for j in range(tensors):
            do_ref[j] = dot(dat, wt_ref[0, j, :, 3 * width :]).astype(BF)
            gwt_ref[j] = dot(dat, ot_ref[j], TN).astype(BF)
        sv_ref[...] = jnp.zeros_like(sv_ref)
        sv_ref[0:1, :] = dg
        sv_ref[1:2, :] = db
        sv_ref[2:3, :] = jnp.sum(gm, axis=0, keepdims=True)


def whole(shape):
    zero = (0,) * len(shape)
    return pl.BlockSpec(shape, lambda *_: zero)


def call(body, grid, ins, in_specs, outs, out_specs, scratch, prefetch=0, name=None):
    return pl.pallas_call(
        body,
        out_shape=tuple(jax.ShapeDtypeStruct(s, d) for s, d in outs),
        grid_spec=pltpu.PrefetchScalarGridSpec(
            num_scalar_prefetch=prefetch,
            grid=(grid,),
            in_specs=in_specs,
            out_specs=tuple(out_specs),
            scratch_shapes=scratch,
        ),
        compiler_params=pltpu.CompilerParams(
            dimension_semantics=("arbitrary",), vmem_limit_bytes=60 * 1024 * 1024
        ),
        name=name,
    )(*ins)


def swap_core(v):
    size = lax.axis_size("tensor")
    return lax.ppermute(v, "tensor", [(i, i ^ 1) for i in range(size)])


def shards(
    tokens, query_space, key_space, value_space, output_space, query_time, key_time, value_time,
    output_time, mlp_in, bias_in, mlp_out, bias_out, gain_first, shift_first, gain_second,
    shift_second, gain_third, shift_third, place_slot, cotangent,
):
    F = lax.axis_size("frame")
    T = lax.axis_size("tensor")
    clips, frames_dev, places_dev, D = tokens.shape
    width = query_space.shape[1]
    heads = width // HEAD
    hid = mlp_in.shape[1]
    rows_w = query_space.shape[0]
    fr = clips * frames_dev // T
    fp = frames_dev // fr
    R = fr * T * PAD
    f_id = lax.axis_index("frame")
    t_id = lax.axis_index("tensor")
    core = t_id % 2

    def pack(q, k, v, o):
        return jnp.concatenate((q, k, v, o.T), axis=1)

    wl = jnp.stack(
        (
            pack(query_space, key_space, value_space, output_space),
            pack(query_time, key_time, value_time, output_time),
            mlp_in,
            mlp_out.T,
        )
    )
    part_bin = lax.dynamic_slice(bias_in, (f_id * (hid // F),), (hid // F,)).astype(F32)
    part_bout = lax.dynamic_slice(
        bias_out, (t_id * (bias_out.shape[0] // T),), (bias_out.shape[0] // T,)
    ).astype(F32)
    small = jnp.concatenate(
        (gain_first, shift_first, gain_second, shift_second, gain_third, shift_third, part_bout, part_bin)
    )
    FT = ("frame", "tensor")
    small_all = lax.all_gather(small, FT, axis=0, tiled=False)
    nv = 7 * gain_first.shape[0]
    vec = small_all[:, :nv].reshape(F * T, 7, -1).transpose(1, 0, 2).reshape(7, D)
    vec = jnp.concatenate((vec, jnp.zeros((1, D), F32)), axis=0)
    bin_all = small_all[:, nv:].reshape(F, T, -1).transpose(1, 0, 2).reshape(T, hid)
    W = lax.all_gather(wl, FT, axis=0, tiled=False).reshape(F, T, 4, rows_w, D)
    W = W.transpose(2, 1, 0, 3, 4).reshape(4, T, F * rows_w, D)

    def to_owner(v):
        v = jnp.pad(v, ((0, 0), (0, 0), (0, PAD - places_dev), (0, 0)))
        v = v.reshape(T, fr, PAD, D)
        v = lax.all_to_all(v, "tensor", split_axis=0, concat_axis=0, tiled=True)
        return v.transpose(1, 0, 2, 3).reshape(R, D)

    def from_owner(v):
        v = v.reshape(fr, T, PAD, D).transpose(1, 0, 2, 3)
        v = lax.all_to_all(v, "tensor", split_axis=0, concat_axis=0, tiled=True)
        return v.reshape(clips, frames_dev, PAD, D)[:, :, :places_dev]

    x = to_owner(tokens)
    cot = to_owner(cotangent)
    keep = place_slot >= 0
    bias = jnp.where(keep, 0.0, -1e30).astype(F32).reshape(T, places_dev)
    bias = jnp.pad(bias, ((0, 0), (0, PAD - places_dev)), constant_values=-1e30).reshape(1, T * PAD)
    rows = T * PAD

    qkv_s, os_s, xs, ht = call(
        partial(space_forward, width, heads, fr, rows),
        T,
        (x, vec, bias, W),
        [whole((R, D)), whole((8, D)), whole((1, rows)), pl.BlockSpec((1, 1, D, D), lambda t: (0, t, 0, 0))],
        [((T, R, 3 * width), BF), ((T, R, width), BF), ((R, D), F32), ((R, D), BF)],
        [
            pl.BlockSpec((1, R, 3 * width), lambda t: (t, 0, 0)),
            pl.BlockSpec((1, R, width), lambda t: (t, 0, 0)),
            whole((R, D)),
            whole((R, D)),
        ],
        [pltpu.VMEM((R, D), BF)],
        name="space_forward",
    )

    groups = PAD // 8
    nf = 2 * F * fr
    size = nf * 8
    RT = groups * size

    def to_time(own):
        v = own.transpose(1, 0, 2, 3)
        return lax.all_to_all(v, "frame", split_axis=0, concat_axis=0, tiled=True)

    def group_rows(a, b):
        v = jnp.stack((a, b)).reshape(nf, groups, 8, a.shape[-1])
        return v.transpose(1, 0, 2, 3).reshape(RT, a.shape[-1])

    def ungroup_rows(v):
        n = v.shape[-1]
        return v.reshape(groups, nf, 8, n).transpose(1, 0, 2, 3).reshape(2, F, fr, PAD, n)

    def to_frames(v):
        v = lax.all_to_all(v, "frame", split_axis=0, concat_axis=0, tiled=True)
        return v.transpose(1, 0, 2, 3).reshape(R, v.shape[-1])

    h_own = to_time(ht.reshape(fr, T, PAD, D))
    h_t = group_rows(h_own, swap_core(h_own))
    keep_q = lax.dynamic_slice(
        jnp.pad(keep.astype(F32).reshape(T, places_dev), ((0, 0), (0, PAD - places_dev))), (f_id, 0), (1, PAD)
    )
    mask = jnp.broadcast_to(keep_q.reshape(groups, 1, 8), (groups, nf, 8)).reshape(RT, 1)
    core_arr = core.reshape(1).astype(jnp.int32)
    halves = T // 2
    time_w = pl.BlockSpec((1, 1, D, D), lambda i, c: (1, c[0] + 2 * i, 0, 0))
    per_half = lambda n: pl.BlockSpec((1, RT, n), lambda i, c: (i, 0, 0))
    qkv_t, ot = call(
        partial(time_forward, width, heads, groups, size, 8),
        halves,
        (core_arr, h_t, W, mask),
        [whole((RT, D)), time_w, whole((RT, 1))],
        [((halves, RT, 3 * width), BF), ((halves, RT, width), BF)],
        [per_half(3 * width), per_half(width)],
        [],
        prefetch=1,
        name="time_forward",
    )
    ot_u = jnp.stack([ungroup_rows(ot[i]) for i in range(halves)], axis=-2)
    ot_u = ot_u.reshape(2, F, fr, PAD, halves * width)
    ot_mine, ot_other = to_frames(ot_u[0]), to_frames(swap_core(ot_u[1]))

    def by_tensor(mine, other):
        m = mine.reshape(R, halves, width)
        o = other.reshape(R, halves, width)
        first = jnp.where(core == 0, m, o)
        second = jnp.where(core == 0, o, m)
        return jnp.stack((first, second), axis=2).reshape(R, T, width).transpose(1, 0, 2)

    ot_all = by_tensor(ot_mine, ot_other)
    win_spec = lambda kind: pl.BlockSpec((1, 1, D, D), lambda t: (kind, t, 0, 0))
    res, gt, dot_all, g_in, g_out, g_wt, sv_m, gb = call(
        partial(mlp_both, width, T),
        T,
        (xs, cot, ot_all, vec, bin_all, W, W, W),
        [
            whole((R, D)), whole((R, D)), whole((T, R, width)), whole((8, D)), whole((T, hid)),
            pl.BlockSpec((1, T, D, D), lambda t: (1, 0, 0, 0)), win_spec(2), win_spec(3),
        ],
        [
            ((R, D), BF), ((R, D), F32), ((T, R, width), BF), ((T, D, hid), BF), ((T, D, hid), BF),
            ((T, D, width), BF), ((8, D), F32), ((T, hid), F32),
        ],
        [
            whole((R, D)), whole((R, D)), whole((T, R, width)),
            pl.BlockSpec((1, D, hid), lambda t: (t, 0, 0)), pl.BlockSpec((1, D, hid), lambda t: (t, 0, 0)),
            whole((T, D, width)), whole((8, D)), whole((T, hid)),
        ],
        [pltpu.VMEM((R, D), F32), pltpu.VMEM((R, D), BF), pltpu.VMEM((R, D), F32), pltpu.VMEM((R, D), F32)],
        name="mlp_both",
    )
    d = dot_all.reshape(halves, 2, R, width)
    d_mine = jnp.where(core == 0, d[:, 0], d[:, 1])
    d_other = jnp.where(core == 0, d[:, 1], d[:, 0])
    as_frames = lambda v: v.transpose(1, 0, 2).reshape(fr, T, PAD, halves * width)
    d_own = to_time(as_frames(d_mine))
    d_par = to_time(swap_core(as_frames(d_other)))
    d_t = group_rows(d_own, d_par).reshape(RT, halves, width).transpose(1, 0, 2)
    g_time, dh_part = call(
        partial(time_backward, width, heads, groups, size, 8),
        halves,
        (core_arr, h_t, W, mask, qkv_t, d_t),
        [whole((RT, D)), time_w, whole((RT, 1)), per_half(3 * width), per_half(width)],
        [((halves, D, 3 * width), BF), ((RT, D), F32)],
        [pl.BlockSpec((1, D, 3 * width), lambda i, c: (i, 0, 0)), whole((RT, D))],
        [pltpu.VMEM((RT, 3 * width), BF)],
        prefetch=1,
        name="time_backward",
    )
    dh_u = ungroup_rows(dh_part)
    dh_sum = (dh_u[0] + swap_core(dh_u[1].astype(BF)).astype(F32)).astype(BF)
    dht = to_frames(dh_sum)

    gx, g_space, sv_s = call(
        partial(space_backward, width, heads, fr, rows),
        T,
        (x, xs, gt, dht, vec, bias, W, qkv_s, os_s),
        [
            whole((R, D)), whole((R, D)), whole((R, D)), whole((R, D)), whole((8, D)), whole((1, rows)),
            pl.BlockSpec((1, 1, D, D), lambda t: (0, t, 0, 0)),
            pl.BlockSpec((1, R, 3 * width), lambda t: (t, 0, 0)),
            pl.BlockSpec((1, R, width), lambda t: (t, 0, 0)),
        ],
        [((R, D), BF), ((T, D, D), BF), ((8, D), F32)],
        [whole((R, D)), pl.BlockSpec((1, D, D), lambda t: (t, 0, 0)), whole((8, D))],
        [
            pltpu.VMEM((R, D), BF), pltpu.VMEM((R, D), F32), pltpu.VMEM((R, D), BF), pltpu.VMEM((R, D), F32),
            pltpu.VMEM((R, 3 * width), BF),
        ],
        name="space_backward",
    )
    zero = jnp.zeros_like(g_time)
    g_first = jnp.where(core == 0, g_time, zero)
    g_second = jnp.where(core == 0, zero, g_time)
    g_qkv = jnp.stack((g_first, g_second), axis=1).reshape(T, D, 3 * width)
    part = jnp.stack((g_space, jnp.concatenate((g_qkv, g_wt), axis=2), g_in, g_out))
    part = part.reshape(4, T, F, rows_w, D).transpose(2, 1, 0, 3, 4).reshape(F * T, 4, rows_w, D)
    share = lax.psum_scatter(part, FT, scatter_dimension=0, tiled=False)
    share = lax.psum(share.astype(F32), "rep")
    smalls = jnp.concatenate((sv_s[0:4], sv_m[0:3], gb), axis=0)
    smalls = lax.psum(smalls, ("rep", "frame", "tensor"))

    def unpack(g):
        return g[:, :width], g[:, width : 2 * width], g[:, 2 * width : 3 * width], g[:, 3 * width :].T

    gs_q, gs_k, gs_v, gs_o = unpack(share[0])
    gt_q, gt_k, gt_v, gt_o = unpack(share[1])
    n = gain_first.shape[0]
    at = (f_id * T + t_id) * n
    own = lambda row: lax.dynamic_slice(smalls[row], (at,), (n,))
    nb = bias_out.shape[0]
    return (
        from_owner(res),
        from_owner(gx).astype(F32),
        gs_q, gs_k, gs_v, gs_o,
        gt_q, gt_k, gt_v, gt_o,
        share[2],
        lax.dynamic_slice(smalls, (7 + t_id, 0), (1, hid))[0],
        share[3].T,
        lax.dynamic_slice(smalls[6], (f_id * nb,), (nb,)),
        own(0), own(1), own(2), own(3), own(4), own(5),
    )


def solution(mesh):
    rows = P("rep", "frame", "tensor", None)
    ft, tf, vec = P("frame", "tensor"), P("tensor", "frame"), P(("frame", "tensor"))
    placed = (
        rows, ft, ft, ft, tf, ft, ft, ft, tf, ft, P("tensor"), tf, P("frame"),
        vec, vec, vec, vec, vec, vec, P(), rows,
    )
    return jax.shard_map(
        shards,
        mesh=mesh,
        in_specs=placed,
        out_specs=(
            rows, rows, ft, ft, ft, tf, ft, ft, ft, tf, ft, P("tensor"), tf, P("frame"),
            vec, vec, vec, vec, vec, vec,
        ),
        check_vma=False,
    )
```

```python
from functools import partial

import jax
import jax.numpy as jnp
from jax import lax
from jax.experimental import pallas as pl
from jax.experimental.pallas import tpu as pltpu
from jax.sharding import PartitionSpec as P

HEAD = 64
PAD = 56
BF = jnp.bfloat16
F32 = jnp.float32
NT = (((1,), (1,)), ((), ()))
TN = (((0,), (0,)), ((), ()))
GELU_C = 0.7978845608028654
SCALE = HEAD ** (-0.5)
MESH = pl.DeviceIdType.MESH
KS = 2
SPLIT = 2


def dot(a, b, dims=(((1,), (0,)), ((), ()))):
    return lax.dot_general(a, b, dims, preferred_element_type=F32)


def norm_stats(v):
    m = jnp.mean(v, axis=-1, keepdims=True)
    off = v - m
    s = jnp.mean(off * off, axis=-1, keepdims=True)
    r = lax.rsqrt(s + 1e-06)
    return off * r, r


def norm(v, g, b):
    xhat, _ = norm_stats(v)
    return xhat * g + b


def norm_back(v, g, dy):
    xhat, r = norm_stats(v)
    dyg = dy * g
    mean1 = jnp.mean(dyg, axis=-1, keepdims=True)
    mean2 = jnp.mean(dyg * xhat, axis=-1, keepdims=True)
    dx = r * (dyg - mean1 - xhat * mean2)
    dgain = jnp.sum(dy * xhat, axis=0, keepdims=True)
    dshift = jnp.sum(dy, axis=0, keepdims=True)
    return dx, dgain, dshift


def softmax(s):
    m = jnp.max(s, axis=-1, keepdims=True)
    e = jnp.exp(s - m)
    return e / jnp.sum(e, axis=-1, keepdims=True)


def attend_head(q, k, v, bias):
    s = dot(q, k, NT) * SCALE + bias
    p = softmax(s)
    return dot(p.astype(BF), v).astype(BF)


def attend_head_back(do, q, k, v, bias):
    s = dot(q, k, NT) * SCALE + bias
    p = softmax(s)
    dp = dot(do, v, NT)
    dv = dot(p.astype(BF), do, TN)
    inner = jnp.sum(dp * p, axis=-1, keepdims=True)
    ds = (p * (dp - inner)).astype(BF)
    dq = dot(ds, k) * SCALE
    dk = dot(ds, q, TN) * SCALE
    return dq.astype(BF), dk.astype(BF), dv.astype(BF)


def space_forward(width, heads, frames, rows, x_ref, vec_ref, bias_ref, w_ref, qkv_ref, os_ref, xs_ref, ht_ref, h_scr):
    t = pl.program_id(0)

    @pl.when(t == 0)
    def _():
        x = x_ref[...].astype(F32)
        h_scr[...] = norm(x, vec_ref[0:1, :], vec_ref[1:2, :]).astype(BF)
        xs_ref[...] = x

    qkv_ref[0] = dot(h_scr[...], w_ref[0, 0, :, : 3 * width]).astype(BF)
    bias = bias_ref[...]
    for i in range(frames):
        r = pl.ds(i * rows, rows)
        for h in range(heads):
            q = qkv_ref[0, r, h * HEAD : (h + 1) * HEAD]
            k = qkv_ref[0, r, width + h * HEAD : width + (h + 1) * HEAD]
            v = qkv_ref[0, r, 2 * width + h * HEAD : 2 * width + (h + 1) * HEAD]
            os_ref[0, r, h * HEAD : (h + 1) * HEAD] = attend_head(q, k, v, bias)
    xs_ref[...] += dot(os_ref[0], w_ref[0, 0, :, 3 * width :], NT)

    @pl.when(t == pl.num_programs(0) - 1)
    def _():
        ht_ref[...] = norm(xs_ref[...], vec_ref[2:3, :], vec_ref[3:4, :]).astype(BF)


def space_backward(
    width, heads, frames, rows,
    x_ref, xs_ref, gt_ref, dht_ref, vec_ref, bias_ref, w_ref, qkv_ref, os_ref,
    gx_ref, gw_ref, sv_ref, h_scr, gs_scr, dat_scr, dh_scr, dqkv_scr,
):
    t = pl.program_id(0)

    @pl.when(t == 0)
    def _():
        x = x_ref[...].astype(F32)
        h_scr[...] = norm(x, vec_ref[0:1, :], vec_ref[1:2, :]).astype(BF)
        dx, dg, db = norm_back(xs_ref[...], vec_ref[2:3, :], dht_ref[...].astype(F32))
        gs = gt_ref[...] + dx
        gs_scr[...] = gs
        dat_scr[...] = gs.astype(BF)
        sv_ref[2:3, :] = dg
        sv_ref[3:4, :] = db
        sv_ref[4:8, :] = jnp.zeros((4, sv_ref.shape[1]), F32)
        dh_scr[...] = jnp.zeros_like(dh_scr)

    dat = dat_scr[...]
    dos = dot(dat, w_ref[0, 0, :, 3 * width :]).astype(BF)
    bias = bias_ref[...]
    for i in range(frames):
        r = pl.ds(i * rows, rows)
        for h in range(heads):
            a, b, c = (slice(j * width + h * HEAD, j * width + (h + 1) * HEAD) for j in range(3))
            dq, dk, dv = attend_head_back(
                dos[i * rows : (i + 1) * rows, a], qkv_ref[0, r, a], qkv_ref[0, r, b], qkv_ref[0, r, c], bias
            )
            dqkv_scr[r, a] = dq
            dqkv_scr[r, b] = dk
            dqkv_scr[r, c] = dv
    dqkv = dqkv_scr[...]
    gw_ref[0, :, : 3 * width] = dot(h_scr[...], dqkv, TN).astype(BF)
    gw_ref[0, :, 3 * width :] = dot(dat, os_ref[0], TN).astype(BF)
    dh_scr[...] += dot(dqkv, w_ref[0, 0, :, : 3 * width], NT)

    @pl.when(t == pl.num_programs(0) - 1)
    def _():
        dx, dg, db = norm_back(x_ref[...].astype(F32), vec_ref[0:1, :], dh_scr[...])
        gx_ref[...] = (gs_scr[...] + dx).astype(gx_ref.dtype)
        sv_ref[0:1, :] = dg
        sv_ref[1:2, :] = db


def group_bias(size, places):
    i = lax.broadcasted_iota(jnp.int32, (size, size), 0)
    j = lax.broadcasted_iota(jnp.int32, (size, size), 1)
    return jnp.where(i % places == j % places, 0.0, -1e30).astype(F32)


def time_forward(width, heads, groups, size, places, core_ref, h_ref, w_ref, mask_ref, qkv_ref, ot_ref):
    qkv_ref[0] = dot(h_ref[...], w_ref[0, 0, :, : 3 * width]).astype(BF)
    bias = group_bias(size, places)

    def one(g, carry):
        r = pl.ds(pl.multiple_of(g * size, size), size)
        keep = mask_ref[r, :]
        for h in range(heads):
            a, b, c = (slice(j * width + h * HEAD, j * width + (h + 1) * HEAD) for j in range(3))
            s = dot(qkv_ref[0, r, a], qkv_ref[0, r, b], NT) * SCALE + bias
            o = dot(softmax(s).astype(BF), qkv_ref[0, r, c])
            ot_ref[0, r, a] = jnp.where(keep > 0, o, 0.0).astype(BF)
        return carry

    lax.fori_loop(0, groups, one, 0)


def time_backward(
    width, heads, groups, size, places, core_ref, h_ref, w_ref, mask_ref, qkv_ref, do_ref, gw_ref, dh_ref, dqkv_scr
):
    bias = group_bias(size, places)

    def one(g, carry):
        r = pl.ds(pl.multiple_of(g * size, size), size)
        keep = mask_ref[r, :]
        for h in range(heads):
            a, b, c = (slice(j * width + h * HEAD, j * width + (h + 1) * HEAD) for j in range(3))
            do = jnp.where(keep > 0, do_ref[0, r, a].astype(F32), 0.0).astype(BF)
            dq, dk, dv = attend_head_back(do, qkv_ref[0, r, a], qkv_ref[0, r, b], qkv_ref[0, r, c], bias)
            dqkv_scr[r, a] = dq
            dqkv_scr[r, b] = dk
            dqkv_scr[r, c] = dv
        return carry

    lax.fori_loop(0, groups, one, 0)
    dqkv = dqkv_scr[...]
    gw_ref[0] = dot(h_ref[...], dqkv, TN).astype(BF)
    dh = dot(dqkv, w_ref[0, 0, :, : 3 * width], NT)

    @pl.when(pl.program_id(0) == 0)
    def _():
        dh_ref[...] = dh

    @pl.when(pl.program_id(0) > 0)
    def _():
        dh_ref[...] += dh


def mlp_both(
    width, tensors,
    xs_ref, cot_ref, ot_ref, vec_ref, bin_ref, wt_ref, win_ref, wout_ref,
    res_ref, gt_ref, do_ref, gin_ref, gout_ref, gwt_ref, sv_ref, gb_ref,
    xt_scr, hm_scr, xm_scr, dhm_scr,
):
    t = pl.program_id(0)

    @pl.when(t == 0)
    def _():
        xt = xs_ref[...]
        for j in range(tensors):
            xt = xt + dot(ot_ref[j], wt_ref[0, j, :, 3 * width :], NT)
        xt_scr[...] = xt
        hm_scr[...] = norm(xt, vec_ref[4:5, :], vec_ref[5:6, :]).astype(BF)
        xm_scr[...] = xt + vec_ref[6:7, :]
        dhm_scr[...] = jnp.zeros_like(dhm_scr)

    hm = hm_scr[...]
    dz = cot_ref[...]
    win = win_ref[0, 0]
    wout = wout_ref[0, 0]
    pre = dot(hm, win) + bin_ref[pl.ds(t, 1), :]
    sq = pre * pre
    th = jnp.tanh(GELU_C * (pre + 0.044715 * (pre * sq)))
    hidden = (0.5 * pre * (1.0 + th)).astype(BF)
    xm_scr[...] += dot(hidden, wout, NT)
    slope = 0.5 * (1.0 + th) + 0.5 * pre * (1.0 - th * th) * (GELU_C * (1.0 + 0.134145 * sq))
    dpre = dot(dz, wout) * slope
    dpre_b = dpre.astype(BF)
    gb_ref[pl.ds(t, 1), :] = jnp.sum(dpre_b.astype(F32), axis=0, keepdims=True)
    gout_ref[0] = dot(dz, hidden, TN).astype(BF)
    gin_ref[0] = dot(hm, dpre_b, TN).astype(BF)
    dhm_scr[...] += dot(dpre_b, win, NT)

    @pl.when(t == pl.num_programs(0) - 1)
    def _():
        res_ref[...] = xm_scr[...].astype(BF)
        gm = dz.astype(F32)
        dx, dg, db = norm_back(xt_scr[...], vec_ref[4:5, :], dhm_scr[...])
        gt = gm + dx
        gt_ref[...] = gt
        dat = gt.astype(BF)
        for j in range(tensors):
            do_ref[j] = dot(dat, wt_ref[0, j, :, 3 * width :]).astype(BF)
            gwt_ref[j] = dot(dat, ot_ref[j], TN).astype(BF)
        sv_ref[...] = jnp.zeros_like(sv_ref)
        sv_ref[0:1, :] = dg
        sv_ref[1:2, :] = db
        sv_ref[2:3, :] = jnp.sum(gm, axis=0, keepdims=True)


def whole(shape):
    zero = (0,) * len(shape)
    return pl.BlockSpec(shape, lambda *_: zero)


def call(body, grid, ins, in_specs, outs, out_specs, scratch, prefetch=0, name=None):
    return pl.pallas_call(
        body,
        out_shape=tuple(jax.ShapeDtypeStruct(s, d) for s, d in outs),
        grid_spec=pltpu.PrefetchScalarGridSpec(
            num_scalar_prefetch=prefetch,
            grid=(grid,),
            in_specs=in_specs,
            out_specs=tuple(out_specs),
            scratch_shapes=scratch,
        ),
        compiler_params=pltpu.CompilerParams(
            dimension_semantics=("arbitrary",), vmem_limit_bytes=60 * 1024 * 1024
        ),
        name=name,
    )(*ins)


def row_views(refs, outs, to_owner, n, mine, theirs):
    if to_owner:
        return refs[n].at[theirs], outs[n].at[:, mine]
    return refs[n].at[:, theirs], outs[n].at[mine]


def rows_start(T, t, rc, refs, outs, to_owner, rs, rr, rl):
    for n in range(len(refs)):
        for p in range(1, T):
            src, dst = row_views(refs, outs, to_owner, n, t, t ^ p)
            rc(src, dst, rs.at[n, p], rr.at[n, p], tensor=t ^ p).start()
        src, dst = row_views(refs, outs, to_owner, n, t, t)
        pltpu.make_async_copy(src, dst, rl.at[n]).start()


def rows_wait(T, t, rc, refs, outs, to_owner, rs, rr, rl):
    for n in range(len(refs)):
        for p in range(1, T):
            src, _ = row_views(refs, outs, to_owner, n, t, t ^ p)
            _, dst = row_views(refs, outs, to_owner, n, t ^ p, t)
            c = rc(src, dst, rs.at[n, p], rr.at[n, p], tensor=t ^ p)
            c.wait_send()
            c.wait_recv()
        src, dst = row_views(refs, outs, to_owner, n, t, t)
        pltpu.make_async_copy(src, dst, rl.at[n]).wait()


def gather_kernel(F, T, K, KS, w_ref, s_ref, a_ref, b_ref, W_ref, S_ref, ao_ref, bo_ref, loc_sem, zs, zr, ys, yr, xs, xr, cs, cr, ss, sr, rs, rr, rl):
    r, f, t = lax.axis_index("rep"), lax.axis_index("frame"), lax.axis_index("tensor")
    rows = w_ref.shape[1]
    half = rows // 2
    core, ypart, xpart = t ^ 1, t ^ 2, r ^ 1
    mine = pl.ds(pl.multiple_of((r % 2) * half, half), half)
    other = pl.ds(pl.multiple_of((1 - r % 2) * half, half), half)

    def rc(src, dst, ssem, rsem, **dev):
        return pltpu.make_async_remote_copy(src, dst, ssem, rsem, device_id=dev, device_id_type=MESH)

    bar = pltpu.get_barrier_semaphore()
    for d in range(1, F):
        for peer in (f - d, f + d):
            @pl.when((peer >= 0) & (peer < F))
            def _():
                pl.semaphore_signal(bar, inc=1, device_id={"frame": peer}, device_id_type=MESH)
    pl.semaphore_signal(bar, inc=1, device_id={"tensor": core}, device_id_type=MESH)
    pl.semaphore_signal(bar, inc=1, device_id={"tensor": ypart}, device_id_type=MESH)
    pl.semaphore_signal(bar, inc=1, device_id={"tensor": t ^ 3}, device_id_type=MESH)
    pl.semaphore_signal(bar, inc=1, device_id={"rep": xpart}, device_id_type=MESH)
    pl.semaphore_wait(bar, F + 3)

    def blk(k, tt, src, part=None):
        return W_ref.at[k, tt, src] if part is None else W_ref.at[k, tt, src, part]

    def zpart(k):
        return None if k < KS else mine

    def z_copy(k, src, to):
        ref = blk(k, t, src, zpart(k))
        return rc(ref, ref, zs.at[k, src, jnp.where(to > f, 1, 0)], zr.at[k, src], frame=to)

    def z_own(k, to):
        s = w_ref.at[k] if k < KS else w_ref.at[k, mine]
        return rc(s, blk(k, t, f, zpart(k)), zs.at[k, f, jnp.where(to > f, 1, 0)], zr.at[k, f], frame=to)

    def y_copy(k, src, own):
        s = w_ref.at[k, mine] if own else W_ref.at[k, t, src, mine]
        return rc(s, W_ref.at[k, t, src, mine], ys.at[k, src], yr.at[k, src], tensor=ypart)

    def y_in(k, src):
        ref = W_ref.at[k, ypart, src, mine]
        return rc(ref, ref, ys.at[k, src], yr.at[k, src], tensor=ypart)

    def x_copy(k, src, part):
        ref = W_ref.at[k, ypart, src, part]
        return rc(ref, ref, xs.at[k, src], xr.at[k, src], rep=xpart)

    def xo_copy(k, src, part):
        ref = W_ref.at[k, t, src, part]
        return rc(ref, ref, xs.at[K + k, src], xr.at[K + k, src], rep=xpart)

    def c_copy(j, k, src, tt, own=False):
        if j >= 3:
            dst = W_ref.at[k, tt, src, mine if j == 3 else other]
            return rc(dst, dst, cs.at[j, k, src], cr.at[j, k, src], tensor=core)
        if j == 0:
            dst = W_ref.at[k, tt, src]
            return rc(w_ref.at[k] if own else dst, dst, cs.at[0, k, src], cr.at[0, k, src], tensor=core)
        part = mine if j == 1 else other
        dst = W_ref.at[k, tt, src, part]
        return rc(dst, dst, cs.at[j, k, src], cr.at[j, k, src], tensor=core)

    def small(i, dst, src, **dev):
        return rc(src, dst, ss.at[i], sr.at[i], **dev)

    def each(d, fn):
        if d == 0:
            fn(f, 0)
        else:
            for sign in (-1, 1):
                src = f + sign * d
                @pl.when((src >= 0) & (src < F))
                def _():
                    fn(src, sign)

    for k in range(K):
        for to in (f - 1, f + 1):
            @pl.when((to >= 0) & (to < F))
            def _():
                z_own(k, to).start()
        y_copy(k, f, True).start()
    for k in range(K):
        c_copy(0, k, f, t, own=True).start()
        pltpu.make_async_copy(w_ref.at[k], W_ref.at[k, t, f], loc_sem.at[k]).start()
    for d in range(1, F):
        for sign in (-1, 1):
            to = f + sign * d
            @pl.when((to >= 0) & (to < F))
            def _():
                rc(s_ref, S_ref.at[t, f], ss.at[to], sr.at[f], frame=to).start()
    pltpu.make_async_copy(s_ref, S_ref.at[t, f], loc_sem.at[K]).start()
    pltpu.make_async_copy(s_ref, S_ref.at[t, f], loc_sem.at[K]).wait()

    def z_step(k, d):
        def fn(src, sign):
            z_copy(k, src, f).wait_recv()
            to = f - sign
            @pl.when((to >= 0) & (to < F))
            def _():
                z_copy(k, src, to).start()
            y_copy(k, src, False).start()
            if k < KS:
                c_copy(0, k, src, t).start()
            else:
                xo_copy(k, src, mine).start()
                c_copy(3, k, src, t).start()
        each(d, fn)

    def y_step(k, d):
        def fn(src, sign):
            y_in(k, src).wait_recv()
            x_copy(k, src, mine).start()
            c_copy(1, k, src, ypart).start()
        each(d, fn)

    def x_step(k, d):
        def fn(src, sign):
            x_copy(k, src, other).wait_recv()
            c_copy(2, k, src, ypart).start()
            if k >= KS and sign != 0:
                xo_copy(k, src, other).wait_recv()
                c_copy(4, k, src, t).start()
        each(d, fn)

    for d in range(F):
        for k in range(K):
            if d > 0:
                z_step(k, d)
            y_step(k, d)
            if d > 0:
                x_step(k, d - 1)
        if d == 1:
            rows_start(T, t, rc, (a_ref, b_ref), (ao_ref, bo_ref), True, rs, rr, rl)
            for dd in range(1, F):
                def fn(src, sign):
                    rc(s_ref, S_ref.at[t, src], ss.at[src], sr.at[src], frame=f).wait_recv()
                each(dd, fn)
            rc(S_ref.at[t], S_ref.at[t], ss.at[F], sr.at[F], tensor=ypart).start()
        if d == 2:
            rc(S_ref.at[ypart], S_ref.at[ypart], ss.at[F], sr.at[F], tensor=ypart).wait_recv()
            rc(S_ref.at[t], S_ref.at[t], ss.at[F + 1], sr.at[F + 1], tensor=core).start()
            rc(S_ref.at[ypart], S_ref.at[ypart], ss.at[F + 2], sr.at[F + 2], tensor=core).start()
    for k in range(K):
        x_step(k, F - 1)
    rows_wait(T, t, rc, (a_ref, b_ref), (ao_ref, bo_ref), True, rs, rr, rl)
    ct, cy = core, core ^ 2
    for k in range(K):
        pltpu.make_async_copy(w_ref.at[k], W_ref.at[k, t, f], loc_sem.at[k]).wait()
        for d in range(F):
            def fn(src, sign):
                if k < KS or sign == 0:
                    c_copy(0, k, src, ct).wait_recv()
                    c_copy(0, k, src, t).wait_send()
                else:
                    for j in (3, 4):
                        c_copy(j, k, src, ct).wait_recv()
                        c_copy(j, k, src, t).wait_send()
                    xo_copy(k, src, mine).wait_send()
                c_copy(1, k, src, cy).wait_recv()
                c_copy(2, k, src, cy).wait_recv()
                c_copy(1, k, src, ypart).wait_send()
                c_copy(2, k, src, ypart).wait_send()
                y_copy(k, src, False).wait_send()
                x_copy(k, src, mine).wait_send()
                if sign == 0:
                    for to in (f - 1, f + 1):
                        @pl.when((to >= 0) & (to < F))
                        def _():
                            z_own(k, to).wait_send()
                else:
                    to = f - sign
                    @pl.when((to >= 0) & (to < F))
                    def _():
                        z_copy(k, src, to).wait_send()
            each(d, fn)
    for dd in range(1, F):
        def fn(src, sign):
            rc(s_ref, S_ref.at[t, f], ss.at[src], sr.at[f], frame=src).wait_send()
        each(dd, fn)
    rc(S_ref.at[t], S_ref.at[t], ss.at[F], sr.at[F], tensor=ypart).wait_send()
    rc(S_ref.at[t], S_ref.at[t], ss.at[F + 1], sr.at[F + 1], tensor=core).wait_send()
    rc(S_ref.at[ypart], S_ref.at[ypart], ss.at[F + 2], sr.at[F + 2], tensor=core).wait_send()
    rc(S_ref.at[ct], S_ref.at[ct], ss.at[F + 1], sr.at[F + 1], tensor=core).wait_recv()
    rc(S_ref.at[cy], S_ref.at[cy], ss.at[F + 2], sr.at[F + 2], tensor=core).wait_recv()


def gather_all(wl, small, a, b):
    F, T = lax.axis_size("frame"), lax.axis_size("tensor")
    K, rows, D = wl.shape
    dma = pltpu.SemaphoreType.DMA
    any_spec = pl.BlockSpec(memory_space=pl.ANY)
    owned = (a.shape[1], a.shape[0]) + a.shape[2:]
    sds = jax.ShapeDtypeStruct
    return pl.pallas_call(
        partial(gather_kernel, F, T, K, KS),
        out_shape=(
            sds((K, T, F, rows, D), wl.dtype), sds((T, F) + small.shape, small.dtype),
            sds(owned, a.dtype), sds(owned, b.dtype),
        ),
        in_specs=[pl.BlockSpec(memory_space=pltpu.VMEM)] * 4,
        out_specs=(any_spec,) * 4,
        scratch_shapes=[
            dma((K + 1,)), dma((K, F, 2)), dma((K, F)), dma((K, F)), dma((K, F)), dma((2 * K, F)), dma((2 * K, F)),
            dma((5, K, F)), dma((5, K, F)), dma((F + 3,)), dma((F + 3,)), dma((2, T)), dma((2, T)), dma((2,)),
        ],
        compiler_params=pltpu.CompilerParams(collective_id=0, has_side_effects=True, vmem_limit_bytes=16 * 1024 * 1024),
        name="gather_all",
    )(wl, small, a, b)


def reduce_kernel(F, T, G, split, *refs):
    g_refs, s_ref, a_ref, b_ref = refs[:G], *refs[G : G + 3]
    out_ref, sout_ref, ao_ref, bo_ref = refs[G + 3 : G + 7]
    (acc, cin, xin, yin, zdn, zup, fin, sacc, scin, sxin, syin, szin,
     lsem, cs, cr, xs, xr, ys, yr, zs, zr, fs, fr_, ss, sr, rs, rr, rl) = refs[G + 7 :]
    K = G * split
    r, f, t = lax.axis_index("rep"), lax.axis_index("frame"), lax.axis_index("tensor")
    rows = acc.shape[3]
    half = rows // 2
    core, ypart, xpart = t ^ 1, t ^ 2, r ^ 1
    mine = pl.ds(pl.multiple_of((r % 2) * half, half), half)
    other = pl.ds(pl.multiple_of((1 - r % 2) * half, half), half)

    def rc(src, dst, ssem, rsem, **dev):
        return pltpu.make_async_remote_copy(src, dst, ssem, rsem, device_id=dev, device_id_type=MESH)

    bar = pltpu.get_barrier_semaphore()
    for d in range(1, F):
        for peer in (f - d, f + d):
            @pl.when((peer >= 0) & (peer < F))
            def _():
                pl.semaphore_signal(bar, inc=1, device_id={"frame": peer}, device_id_type=MESH)
    pl.semaphore_signal(bar, inc=1, device_id={"tensor": core}, device_id_type=MESH)
    pl.semaphore_signal(bar, inc=1, device_id={"tensor": ypart}, device_id_type=MESH)
    pl.semaphore_signal(bar, inc=1, device_id={"tensor": t ^ 3}, device_id_type=MESH)
    pl.semaphore_signal(bar, inc=1, device_id={"rep": xpart}, device_id_type=MESH)
    pl.semaphore_wait(bar, F + 3)

    def source(k, tt):
        return g_refs[k // split].at[tt, :, pl.ds((k % split) * rows, rows)]

    def load(k, j):
        return pltpu.make_async_copy(source(k, t if j == 0 else ypart), acc.at[k, j], lsem.at[k, j])

    def c_copy(k, j):
        return rc(source(k, core if j == 0 else core ^ 2), cin.at[k, j], cs.at[k, j], cr.at[k, j], tensor=core)

    def x_copy(k):
        return rc(acc.at[k, 1, :, other], xin.at[k], xs.at[k], xr.at[k], rep=xpart)

    def y_copy(k):
        return rc(acc.at[k, 1, :, mine], yin.at[k], ys.at[k], yr.at[k], tensor=ypart)

    def z_copy(k, dst, down):
        buf = zdn if down else zup
        return rc(acc.at[k, 0, dst], buf.at[k, dst], zs.at[k, dst], zr.at[k, dst, 0 if down else 1],
                  frame=f - 1 if down else f + 1)

    def fin_copy(k):
        return rc(acc.at[k, 0, f], fin.at[k], fs.at[k], fr_.at[k], rep=xpart)

    def small_copy(i):
        if i == 0:
            return rc(s_ref.at[pl.ds(0, 2), 1 - t % 2], scin, ss.at[0], sr.at[0], tensor=core)
        if i == 1:
            return rc(sacc, sxin, ss.at[1], sr.at[1], rep=xpart)
        return rc(sacc.at[1 - t // 2], syin, ss.at[2], sr.at[2], tensor=ypart)

    def small_frames(fn):
        for d in range(1, F):
            for to in (f - d, f + d):
                @pl.when((to >= 0) & (to < F))
                def _():
                    fn(to)

    def small_step(i):
        if 0 < i < 4:
            small_copy(i - 1).wait()
        if i == 1:
            for yy in range(2):
                sacc[yy] = s_ref[yy, t % 2] + scin[yy]
        elif i == 2:
            sacc[...] += sxin[...]
        elif i == 3:
            syin[...] += sacc[t // 2]
            small_frames(lambda to: rc(syin.at[to], szin.at[f], ss.at[3 + to], sr.at[3 + f], frame=to).start())
        elif i == 4:
            small_frames(lambda to: rc(syin.at[to], szin.at[to], ss.at[3 + to], sr.at[3 + to], frame=to).wait())
            szin[f] = syin[f]
            out = szin[0]
            for n in range(1, F):
                out = out + szin[n]
            sout_ref[...] = out
        if i < 3:
            small_copy(i).start()

    for k in range(K):
        for j in (1, 0):
            c_copy(k, j).start()
            load(k, j).start()
    rows_start(T, t, rc, (a_ref, b_ref), (ao_ref, bo_ref), False, rs, rr, rl)

    def add(k, j):
        c_copy(k, j).wait_recv()
        load(k, j).wait()
        @pl.loop(0, F)
        def _(i):
            acc[k, j, i] = acc[k, j, i] + cin[k, j, i]

    def step_a(k):
        add(k, 1)
        x_copy(k).start()
        add(k, 0)

    def step_b(k):
        x_copy(k).wait()
        @pl.loop(0, F)
        def _(i):
            acc[k, 1, i, mine] = acc[k, 1, i, mine] + xin[k, i]
        y_copy(k).start()

    def step_c(k):
        y_copy(k).wait()
        @pl.loop(0, F)
        def _(i):
            acc[k, 0, i, mine] = acc[k, 0, i, mine] + yin[k, i]
        for dst in range(F):
            @pl.when((f == F - 1) & (dst < f))
            def _():
                z_copy(k, dst, True).start()
            up = F - 1 - dst
            @pl.when((f == 0) & (up > f))
            def _():
                z_copy(k, up, False).start()

    def take(k, dst, down):
        buf = zdn if down else zup
        rc(buf.at[k, dst], buf.at[k, dst], zs.at[k, dst], zr.at[k, dst, 0 if down else 1], frame=f).wait_recv()
        acc[k, 0, dst] = acc[k, 0, dst] + buf[k, dst]
        @pl.when(dst != f)
        def _():
            z_copy(k, dst, down).start()

    def step_d(k):
        for hop in range(1, F):
            @pl.when(f == F - 1 - hop)
            def _():
                for dst in range(F):
                    @pl.when(dst <= f)
                    def _():
                        take(k, dst, True)
            @pl.when(f == hop)
            def _():
                for up in range(F):
                    dst = F - 1 - up
                    @pl.when(dst >= f)
                    def _():
                        take(k, dst, False)
        fin_copy(k).start()

    def step_e(k):
        fin_copy(k).wait()
        part = pl.ds((k % split) * rows, rows)
        out_ref[k // split, part, :] = acc[k, 0, f].astype(F32) + fin[k].astype(F32)

    steps = (step_a, step_b, step_c, step_d, step_e)
    for s in range(K + len(steps) - 1):
        for i, fn in enumerate(steps):
            if 0 <= s - i < K:
                fn(s - i)
        if s < 5:
            small_step(s)
    rows_wait(T, t, rc, (a_ref, b_ref), (ao_ref, bo_ref), False, rs, rr, rl)
    for k in range(K):
        for j in (1, 0):
            c_copy(k, j).wait_send()
        for dst in range(F):
            @pl.when(dst < f)
            def _():
                z_copy(k, dst, True).wait_send()
            @pl.when(dst > f)
            def _():
                z_copy(k, dst, False).wait_send()


def reduce_all(grads, small, a, b):
    F, T = lax.axis_size("frame"), lax.axis_size("tensor")
    G = len(grads)
    K = G * SPLIT
    _, _, full, D = grads[0].shape
    rows = full // SPLIT
    dma = pltpu.SemaphoreType.DMA
    V = pltpu.VMEM
    sm = small.shape[2:]
    sds = jax.ShapeDtypeStruct
    any_spec, vmem = pl.BlockSpec(memory_space=pl.ANY), pl.BlockSpec(memory_space=pltpu.VMEM)
    split_rows = (a.shape[1], a.shape[0]) + a.shape[2:]
    return pl.pallas_call(
        partial(reduce_kernel, F, T, G, SPLIT),
        out_shape=(sds((G, full, D), F32), sds(sm, F32), sds(split_rows, a.dtype), sds(split_rows, b.dtype)),
        in_specs=[any_spec] * G + [vmem] * 3,
        out_specs=(vmem, vmem, any_spec, any_spec),
        scratch_shapes=[
            V((K, 2, F, rows, D), BF), V((K, 2, F, rows, D), BF), V((K, F, rows // 2, D), BF), V((K, F, rows // 2, D), BF),
            V((K, F, rows, D), BF), V((K, F, rows, D), BF), V((K, rows, D), BF),
            V((2, F) + sm, F32), V((2, F) + sm, F32), V((2, F) + sm, F32), V((F,) + sm, F32), V((F,) + sm, F32),
            dma((K, 2)), dma((K, 2)), dma((K, 2)), dma((K,)), dma((K,)), dma((K,)), dma((K,)),
            dma((K, F)), dma((K, F, 2)), dma((K,)), dma((K,)), dma((3 + F,)), dma((3 + F,)),
            dma((2, T)), dma((2, T)), dma((2,)),
        ],
        compiler_params=pltpu.CompilerParams(collective_id=1, has_side_effects=True, vmem_limit_bytes=62 * 1024 * 1024),
        name="reduce_all",
    )(*grads, small.reshape((2, T // 2, F) + sm).astype(F32), a, b)


def swap_core(v):
    size = lax.axis_size("tensor")
    return lax.ppermute(v, "tensor", [(i, i ^ 1) for i in range(size)])


def shards(
    tokens, query_space, key_space, value_space, output_space, query_time, key_time, value_time,
    output_time, mlp_in, bias_in, mlp_out, bias_out, gain_first, shift_first, gain_second,
    shift_second, gain_third, shift_third, place_slot, cotangent,
):
    F = lax.axis_size("frame")
    T = lax.axis_size("tensor")
    clips, frames_dev, places_dev, D = tokens.shape
    width = query_space.shape[1]
    heads = width // HEAD
    hid = mlp_in.shape[1]
    rows_w = query_space.shape[0]
    fr = clips * frames_dev // T
    fp = frames_dev // fr
    R = fr * T * PAD
    f_id = lax.axis_index("frame")
    t_id = lax.axis_index("tensor")
    core = t_id % 2

    def pack(q, k, v, o):
        return jnp.concatenate((q, k, v, o.T), axis=1)

    wl = jnp.stack(
        (
            pack(query_space, key_space, value_space, output_space),
            pack(query_time, key_time, value_time, output_time),
            mlp_in,
            mlp_out.T,
        )
    )
    part_bin = lax.dynamic_slice(bias_in, (f_id * (hid // F),), (hid // F,)).astype(F32)
    part_bout = lax.dynamic_slice(
        bias_out, (t_id * (bias_out.shape[0] // T),), (bias_out.shape[0] // T,)
    ).astype(F32)
    small = jnp.concatenate(
        (gain_first, shift_first, gain_second, shift_second, gain_third, shift_third, part_bout, part_bin)
    )

    def lanes(flat):
        pad = -flat.shape[-1] % 1024
        flat = jnp.pad(flat, [(0, 0)] * (flat.ndim - 1) + [(0, pad)])
        return flat.reshape(flat.shape[:-1] + (-1, 128))

    def split_places(v):
        v = jnp.pad(v, ((0, 0), (0, 0), (0, PAD - places_dev), (0, 0)))
        return v.reshape(T, fr, PAD, D)

    W, small_all, x, cot = gather_all(wl, lanes(small), split_places(tokens), split_places(cotangent))
    W = W.reshape(4, T, F * rows_w, D)
    x, cot = x.reshape(R, D), cot.reshape(R, D)
    small_all = small_all.reshape(T, F, -1)
    nv = 7 * gain_first.shape[0]
    vec = small_all[:, :, :nv].reshape(T, F, 7, -1).transpose(2, 1, 0, 3).reshape(7, D)
    vec = jnp.concatenate((vec, jnp.zeros((1, D), F32)), axis=0)
    bin_all = small_all[:, :, nv : nv + hid // F].reshape(T, hid)

    keep = place_slot >= 0
    bias = jnp.where(keep, 0.0, -1e30).astype(F32).reshape(T, places_dev)
    bias = jnp.pad(bias, ((0, 0), (0, PAD - places_dev)), constant_values=-1e30).reshape(1, T * PAD)
    rows = T * PAD

    qkv_s, os_s, xs, ht = call(
        partial(space_forward, width, heads, fr, rows),
        T,
        (x, vec, bias, W),
        [whole((R, D)), whole((8, D)), whole((1, rows)), pl.BlockSpec((1, 1, D, D), lambda t: (0, t, 0, 0))],
        [((T, R, 3 * width), BF), ((T, R, width), BF), ((R, D), F32), ((R, D), BF)],
        [
            pl.BlockSpec((1, R, 3 * width), lambda t: (t, 0, 0)),
            pl.BlockSpec((1, R, width), lambda t: (t, 0, 0)),
            whole((R, D)),
            whole((R, D)),
        ],
        [pltpu.VMEM((R, D), BF)],
        name="space_forward",
    )

    groups = PAD // 8
    nf = 2 * F * fr
    size = nf * 8
    RT = groups * size

    def to_time(own):
        v = own.transpose(1, 0, 2, 3)
        return lax.all_to_all(v, "frame", split_axis=0, concat_axis=0, tiled=True)

    def group_rows(a, b):
        v = jnp.stack((a, b)).reshape(nf, groups, 8, a.shape[-1])
        return v.transpose(1, 0, 2, 3).reshape(RT, a.shape[-1])

    def ungroup_rows(v):
        n = v.shape[-1]
        return v.reshape(groups, nf, 8, n).transpose(1, 0, 2, 3).reshape(2, F, fr, PAD, n)

    def to_frames(v):
        v = lax.all_to_all(v, "frame", split_axis=0, concat_axis=0, tiled=True)
        return v.transpose(1, 0, 2, 3).reshape(R, v.shape[-1])

    h_own = to_time(ht.reshape(fr, T, PAD, D))
    h_t = group_rows(h_own, swap_core(h_own))
    keep_q = lax.dynamic_slice(
        jnp.pad(keep.astype(F32).reshape(T, places_dev), ((0, 0), (0, PAD - places_dev))), (f_id, 0), (1, PAD)
    )
    mask = jnp.broadcast_to(keep_q.reshape(groups, 1, 8), (groups, nf, 8)).reshape(RT, 1)
    core_arr = core.reshape(1).astype(jnp.int32)
    halves = T // 2
    time_w = pl.BlockSpec((1, 1, D, D), lambda i, c: (1, c[0] + 2 * i, 0, 0))
    per_half = lambda n: pl.BlockSpec((1, RT, n), lambda i, c: (i, 0, 0))
    qkv_t, ot = call(
        partial(time_forward, width, heads, groups, size, 8),
        halves,
        (core_arr, h_t, W, mask),
        [whole((RT, D)), time_w, whole((RT, 1))],
        [((halves, RT, 3 * width), BF), ((halves, RT, width), BF)],
        [per_half(3 * width), per_half(width)],
        [],
        prefetch=1,
        name="time_forward",
    )
    ot_u = jnp.stack([ungroup_rows(ot[i]) for i in range(halves)], axis=-2)
    ot_u = ot_u.reshape(2, F, fr, PAD, halves * width)
    ot_mine, ot_other = to_frames(ot_u[0]), to_frames(swap_core(ot_u[1]))

    def by_tensor(mine, other):
        m = mine.reshape(R, halves, width)
        o = other.reshape(R, halves, width)
        first = jnp.where(core == 0, m, o)
        second = jnp.where(core == 0, o, m)
        return jnp.stack((first, second), axis=2).reshape(R, T, width).transpose(1, 0, 2)

    ot_all = by_tensor(ot_mine, ot_other)
    win_spec = lambda kind: pl.BlockSpec((1, 1, D, D), lambda t: (kind, t, 0, 0))
    res, gt, dot_all, g_in, g_out, g_wt, sv_m, gb = call(
        partial(mlp_both, width, T),
        T,
        (xs, cot, ot_all, vec, bin_all, W, W, W),
        [
            whole((R, D)), whole((R, D)), whole((T, R, width)), whole((8, D)), whole((T, hid)),
            pl.BlockSpec((1, T, D, D), lambda t: (1, 0, 0, 0)), win_spec(2), win_spec(3),
        ],
        [
            ((R, D), BF), ((R, D), F32), ((T, R, width), BF), ((T, D, hid), BF), ((T, D, hid), BF),
            ((T, D, width), BF), ((8, D), F32), ((T, hid), F32),
        ],
        [
            whole((R, D)), whole((R, D)), whole((T, R, width)),
            pl.BlockSpec((1, D, hid), lambda t: (t, 0, 0)), pl.BlockSpec((1, D, hid), lambda t: (t, 0, 0)),
            whole((T, D, width)), whole((8, D)), whole((T, hid)),
        ],
        [pltpu.VMEM((R, D), F32), pltpu.VMEM((R, D), BF), pltpu.VMEM((R, D), F32), pltpu.VMEM((R, D), F32)],
        name="mlp_both",
    )
    d = dot_all.reshape(halves, 2, R, width)
    d_mine = jnp.where(core == 0, d[:, 0], d[:, 1])
    d_other = jnp.where(core == 0, d[:, 1], d[:, 0])
    as_frames = lambda v: v.transpose(1, 0, 2).reshape(fr, T, PAD, halves * width)
    d_own = to_time(as_frames(d_mine))
    d_par = to_time(swap_core(as_frames(d_other)))
    d_t = group_rows(d_own, d_par).reshape(RT, halves, width).transpose(1, 0, 2)
    g_time, dh_part = call(
        partial(time_backward, width, heads, groups, size, 8),
        halves,
        (core_arr, h_t, W, mask, qkv_t, d_t),
        [whole((RT, D)), time_w, whole((RT, 1)), per_half(3 * width), per_half(width)],
        [((halves, D, 3 * width), BF), ((RT, D), F32)],
        [pl.BlockSpec((1, D, 3 * width), lambda i, c: (i, 0, 0)), whole((RT, D))],
        [pltpu.VMEM((RT, 3 * width), BF)],
        prefetch=1,
        name="time_backward",
    )
    dh_u = ungroup_rows(dh_part)
    dh_sum = (dh_u[0] + swap_core(dh_u[1].astype(BF)).astype(F32)).astype(BF)
    dht = to_frames(dh_sum)

    gx, g_space, sv_s = call(
        partial(space_backward, width, heads, fr, rows),
        T,
        (x, xs, gt, dht, vec, bias, W, qkv_s, os_s),
        [
            whole((R, D)), whole((R, D)), whole((R, D)), whole((R, D)), whole((8, D)), whole((1, rows)),
            pl.BlockSpec((1, 1, D, D), lambda t: (0, t, 0, 0)),
            pl.BlockSpec((1, R, 3 * width), lambda t: (t, 0, 0)),
            pl.BlockSpec((1, R, width), lambda t: (t, 0, 0)),
        ],
        [((R, D), BF), ((T, D, D), BF), ((8, D), F32)],
        [whole((R, D)), pl.BlockSpec((1, D, D), lambda t: (t, 0, 0)), whole((8, D))],
        [
            pltpu.VMEM((R, D), BF), pltpu.VMEM((R, D), F32), pltpu.VMEM((R, D), BF), pltpu.VMEM((R, D), F32),
            pltpu.VMEM((R, 3 * width), BF),
        ],
        name="space_backward",
    )
    zero = jnp.zeros_like(g_time)
    g_first = jnp.where(core == 0, g_time, zero)
    g_second = jnp.where(core == 0, zero, g_time)
    g_qkv = jnp.stack((g_first, g_second), axis=1).reshape(T, D, 3 * width)
    kinds = (g_space, jnp.concatenate((g_qkv, g_wt), axis=2), g_in, g_out)
    kinds = tuple(g.reshape(T, F, rows_w, D) for g in kinds)
    n = gain_first.shape[0]
    nb = bias_out.shape[0]
    norms = jnp.concatenate((sv_s[0:4], sv_m[0:2]), axis=0).reshape(6, F, T, n).transpose(2, 1, 0, 3)
    small_g = jnp.concatenate(
        (
            norms.reshape(T, F, 6 * n),
            jnp.broadcast_to(sv_m[2].reshape(1, F, nb), (T, F, nb)),
            jnp.broadcast_to(gb[:, None, :], (T, F, hid)),
        ),
        axis=2,
    )
    share, smalls, res_rows, gx_rows = reduce_all(
        kinds, lanes(small_g), res.reshape(fr, T, PAD, D), gx.reshape(fr, T, PAD, D)
    )
    reps = lax.axis_size("rep")
    if reps > 2:
        share, smalls = (lax.psum(0.5 * v, "rep") for v in (share, smalls))
    smalls = smalls.reshape(-1)

    def join_places(v):
        return v.reshape(clips, frames_dev, PAD, D)[:, :, :places_dev]

    def unpack(g):
        return g[:, :width], g[:, width : 2 * width], g[:, 2 * width : 3 * width], g[:, 3 * width :].T

    gs_q, gs_k, gs_v, gs_o = unpack(share[0])
    gt_q, gt_k, gt_v, gt_o = unpack(share[1])
    own = lambda i: smalls[i * n : (i + 1) * n]
    return (
        join_places(res_rows),
        join_places(gx_rows).astype(F32),
        gs_q, gs_k, gs_v, gs_o,
        gt_q, gt_k, gt_v, gt_o,
        share[2],
        smalls[6 * n + nb : 6 * n + nb + hid],
        share[3].T,
        smalls[6 * n : 6 * n + nb],
        own(0), own(1), own(2), own(3), own(4), own(5),
    )


def solution(mesh):
    rows = P("rep", "frame", "tensor", None)
    ft, tf, vec = P("frame", "tensor"), P("tensor", "frame"), P(("frame", "tensor"))
    placed = (
        rows, ft, ft, ft, tf, ft, ft, ft, tf, ft, P("tensor"), tf, P("frame"),
        vec, vec, vec, vec, vec, vec, P(), rows,
    )
    return jax.shard_map(
        shards,
        mesh=mesh,
        in_specs=placed,
        out_specs=(
            rows, rows, ft, ft, ft, tf, ft, ft, ft, tf, ft, P("tensor"), tf, P("frame"),
            vec, vec, vec, vec, vec, vec,
        ),
        check_vma=False,
    )
```

```python
from functools import partial

import jax
import jax.numpy as jnp
from jax import lax
from jax.experimental import pallas as pl
from jax.experimental.pallas import tpu as pltpu
from jax.sharding import PartitionSpec as P

HEAD = 64
PAD = 56
BF = jnp.bfloat16
F32 = jnp.float32
NT = (((1,), (1,)), ((), ()))
TN = (((0,), (0,)), ((), ()))
GELU_C = 0.7978845608028654
SCALE = HEAD ** (-0.5)
MESH = pl.DeviceIdType.MESH
KS = 1
SPLIT = 2


def dot(a, b, dims=(((1,), (0,)), ((), ()))):
    return lax.dot_general(a, b, dims, preferred_element_type=F32)


def norm_stats(v):
    m = jnp.mean(v, axis=-1, keepdims=True)
    off = v - m
    s = jnp.mean(off * off, axis=-1, keepdims=True)
    r = lax.rsqrt(s + 1e-06)
    return off * r, r


def norm(v, g, b):
    xhat, _ = norm_stats(v)
    return xhat * g + b


def norm_back(v, g, dy):
    xhat, r = norm_stats(v)
    dyg = dy * g
    mean1 = jnp.mean(dyg, axis=-1, keepdims=True)
    mean2 = jnp.mean(dyg * xhat, axis=-1, keepdims=True)
    dx = r * (dyg - mean1 - xhat * mean2)
    dgain = jnp.sum(dy * xhat, axis=0, keepdims=True)
    dshift = jnp.sum(dy, axis=0, keepdims=True)
    return dx, dgain, dshift


def softmax(s):
    m = jnp.max(s, axis=-1, keepdims=True)
    e = jnp.exp(s - m)
    return e / jnp.sum(e, axis=-1, keepdims=True)


def attend_head(q, k, v, bias):
    s = dot(q, k, NT) * SCALE + bias
    p = softmax(s)
    return dot(p.astype(BF), v).astype(BF)


def attend_head_back(do, q, k, v, bias):
    s = dot(q, k, NT) * SCALE + bias
    p = softmax(s)
    dp = dot(do, v, NT)
    dv = dot(p.astype(BF), do, TN)
    inner = jnp.sum(dp * p, axis=-1, keepdims=True)
    ds = (p * (dp - inner)).astype(BF)
    dq = dot(ds, k) * SCALE
    dk = dot(ds, q, TN) * SCALE
    return dq.astype(BF), dk.astype(BF), dv.astype(BF)


def space_forward(width, heads, frames, rows, x_ref, vec_ref, bias_ref, w_ref, qkv_ref, os_ref, xs_ref, ht_ref, h_scr):
    t = pl.program_id(0)

    @pl.when(t == 0)
    def _():
        x = x_ref[...].astype(F32)
        h_scr[...] = norm(x, vec_ref[0:1, :], vec_ref[1:2, :]).astype(BF)
        xs_ref[...] = x

    qkv_ref[0] = dot(h_scr[...], w_ref[0, 0, :, : 3 * width]).astype(BF)
    bias = bias_ref[...]
    for i in range(frames):
        r = pl.ds(i * rows, rows)
        for h in range(heads):
            q = qkv_ref[0, r, h * HEAD : (h + 1) * HEAD]
            k = qkv_ref[0, r, width + h * HEAD : width + (h + 1) * HEAD]
            v = qkv_ref[0, r, 2 * width + h * HEAD : 2 * width + (h + 1) * HEAD]
            os_ref[0, r, h * HEAD : (h + 1) * HEAD] = attend_head(q, k, v, bias)
    xs_ref[...] += dot(os_ref[0], w_ref[0, 0, :, 3 * width :], NT)

    @pl.when(t == pl.num_programs(0) - 1)
    def _():
        ht_ref[...] = norm(xs_ref[...], vec_ref[2:3, :], vec_ref[3:4, :]).astype(BF)


def space_backward(
    width, heads, frames, rows,
    x_ref, xs_ref, gt_ref, dht_ref, vec_ref, bias_ref, w_ref, qkv_ref, os_ref,
    gx_ref, gw_ref, sv_ref, h_scr, gs_scr, dat_scr, dh_scr, dqkv_scr,
):
    t = pl.program_id(0)

    @pl.when(t == 0)
    def _():
        x = x_ref[...].astype(F32)
        h_scr[...] = norm(x, vec_ref[0:1, :], vec_ref[1:2, :]).astype(BF)
        dx, dg, db = norm_back(xs_ref[...], vec_ref[2:3, :], dht_ref[...].astype(F32))
        gs = gt_ref[...] + dx
        gs_scr[...] = gs
        dat_scr[...] = gs.astype(BF)
        sv_ref[2:3, :] = dg
        sv_ref[3:4, :] = db
        sv_ref[4:8, :] = jnp.zeros((4, sv_ref.shape[1]), F32)
        dh_scr[...] = jnp.zeros_like(dh_scr)

    dat = dat_scr[...]
    dos = dot(dat, w_ref[0, 0, :, 3 * width :]).astype(BF)
    bias = bias_ref[...]
    for i in range(frames):
        r = pl.ds(i * rows, rows)
        for h in range(heads):
            a, b, c = (slice(j * width + h * HEAD, j * width + (h + 1) * HEAD) for j in range(3))
            dq, dk, dv = attend_head_back(
                dos[i * rows : (i + 1) * rows, a], qkv_ref[0, r, a], qkv_ref[0, r, b], qkv_ref[0, r, c], bias
            )
            dqkv_scr[r, a] = dq
            dqkv_scr[r, b] = dk
            dqkv_scr[r, c] = dv
    dqkv = dqkv_scr[...]
    gw_ref[0, :, : 3 * width] = dot(h_scr[...], dqkv, TN).astype(BF)
    gw_ref[0, :, 3 * width :] = dot(dat, os_ref[0], TN).astype(BF)
    dh_scr[...] += dot(dqkv, w_ref[0, 0, :, : 3 * width], NT)

    @pl.when(t == pl.num_programs(0) - 1)
    def _():
        dx, dg, db = norm_back(x_ref[...].astype(F32), vec_ref[0:1, :], dh_scr[...])
        gx_ref[...] = (gs_scr[...] + dx).astype(gx_ref.dtype)
        sv_ref[0:1, :] = dg
        sv_ref[1:2, :] = db


def group_bias(size, places):
    i = lax.broadcasted_iota(jnp.int32, (size, size), 0)
    j = lax.broadcasted_iota(jnp.int32, (size, size), 1)
    return jnp.where(i % places == j % places, 0.0, -1e30).astype(F32)


def time_forward(width, heads, groups, size, places, core_ref, h_ref, w_ref, mask_ref, qkv_ref, ot_ref):
    qkv_ref[0] = dot(h_ref[...], w_ref[0, 0, :, : 3 * width]).astype(BF)
    bias = group_bias(size, places)

    def one(g, carry):
        r = pl.ds(pl.multiple_of(g * size, size), size)
        keep = mask_ref[r, :]
        for h in range(heads):
            a, b, c = (slice(j * width + h * HEAD, j * width + (h + 1) * HEAD) for j in range(3))
            s = dot(qkv_ref[0, r, a], qkv_ref[0, r, b], NT) * SCALE + bias
            o = dot(softmax(s).astype(BF), qkv_ref[0, r, c])
            ot_ref[0, r, a] = jnp.where(keep > 0, o, 0.0).astype(BF)
        return carry

    lax.fori_loop(0, groups, one, 0)


def time_backward(
    width, heads, groups, size, places, core_ref, h_ref, w_ref, mask_ref, qkv_ref, do_ref, gw_ref, dh_ref, dqkv_scr
):
    bias = group_bias(size, places)

    def one(g, carry):
        r = pl.ds(pl.multiple_of(g * size, size), size)
        keep = mask_ref[r, :]
        for h in range(heads):
            a, b, c = (slice(j * width + h * HEAD, j * width + (h + 1) * HEAD) for j in range(3))
            do = jnp.where(keep > 0, do_ref[0, r, a].astype(F32), 0.0).astype(BF)
            dq, dk, dv = attend_head_back(do, qkv_ref[0, r, a], qkv_ref[0, r, b], qkv_ref[0, r, c], bias)
            dqkv_scr[r, a] = dq
            dqkv_scr[r, b] = dk
            dqkv_scr[r, c] = dv
        return carry

    lax.fori_loop(0, groups, one, 0)
    dqkv = dqkv_scr[...]
    gw_ref[0] = dot(h_ref[...], dqkv, TN).astype(BF)
    dh = dot(dqkv, w_ref[0, 0, :, : 3 * width], NT)

    @pl.when(pl.program_id(0) == 0)
    def _():
        dh_ref[...] = dh

    @pl.when(pl.program_id(0) > 0)
    def _():
        dh_ref[...] += dh


def mlp_both(
    width, tensors,
    xs_ref, cot_ref, ot_ref, vec_ref, bin_ref, wt_ref, win_ref, wout_ref,
    res_ref, gt_ref, do_ref, gg_ref, gwt_ref, sv_ref, gb_ref,
    xt_scr, hm_scr, xm_scr, dhm_scr,
):
    t = pl.program_id(0)

    @pl.when(t == 0)
    def _():
        xt = xs_ref[...]
        for j in range(tensors):
            xt = xt + dot(ot_ref[j], wt_ref[0, j, :, 3 * width :], NT)
        xt_scr[...] = xt
        hm_scr[...] = norm(xt, vec_ref[4:5, :], vec_ref[5:6, :]).astype(BF)
        xm_scr[...] = xt + vec_ref[6:7, :]
        dhm_scr[...] = jnp.zeros_like(dhm_scr)

    hm = hm_scr[...]
    dz = cot_ref[...]
    lines, _, _, rows, cols = win_ref.shape
    win = win_ref[:, 0, 0].reshape(lines * rows, cols)
    wout = wout_ref[:, 0, 0].reshape(lines * rows, cols)
    pre = dot(hm, win) + bin_ref[pl.ds(t, 1), :]
    sq = pre * pre
    th = jnp.tanh(GELU_C * (pre + 0.044715 * (pre * sq)))
    hidden = (0.5 * pre * (1.0 + th)).astype(BF)
    xm_scr[...] += dot(hidden, wout, NT)
    slope = 0.5 * (1.0 + th) + 0.5 * pre * (1.0 - th * th) * (GELU_C * (1.0 + 0.134145 * sq))
    dpre = dot(dz, wout) * slope
    dpre_b = dpre.astype(BF)
    gb_ref[pl.ds(t, 1), :] = jnp.sum(dpre_b.astype(F32), axis=0, keepdims=True)
    gg_ref[:, 0, 0] = dot(hm, dpre_b, TN).astype(BF).reshape(lines, rows, cols)
    gg_ref[:, 0, 1] = dot(dz, hidden, TN).astype(BF).reshape(lines, rows, cols)
    dhm_scr[...] += dot(dpre_b, win, NT)

    @pl.when(t == pl.num_programs(0) - 1)
    def _():
        res_ref[...] = xm_scr[...].astype(BF)
        gm = dz.astype(F32)
        dx, dg, db = norm_back(xt_scr[...], vec_ref[4:5, :], dhm_scr[...])
        gt = gm + dx
        gt_ref[...] = gt
        dat = gt.astype(BF)
        for j in range(tensors):
            do_ref[j] = dot(dat, wt_ref[0, j, :, 3 * width :]).astype(BF)
            gwt_ref[j] = dot(dat, ot_ref[j], TN).astype(BF)
        sv_ref[...] = jnp.zeros_like(sv_ref)
        sv_ref[0:1, :] = dg
        sv_ref[1:2, :] = db
        sv_ref[2:3, :] = jnp.sum(gm, axis=0, keepdims=True)


def whole(shape):
    zero = (0,) * len(shape)
    return pl.BlockSpec(shape, lambda *_: zero)


def call(body, grid, ins, in_specs, outs, out_specs, scratch, prefetch=0, name=None):
    return pl.pallas_call(
        body,
        out_shape=tuple(jax.ShapeDtypeStruct(s, d) for s, d in outs),
        grid_spec=pltpu.PrefetchScalarGridSpec(
            num_scalar_prefetch=prefetch,
            grid=(grid,),
            in_specs=in_specs,
            out_specs=tuple(out_specs),
            scratch_shapes=scratch,
        ),
        compiler_params=pltpu.CompilerParams(
            dimension_semantics=("arbitrary",), vmem_limit_bytes=60 * 1024 * 1024
        ),
        name=name,
    )(*ins)


def row_views(refs, outs, to_owner, n, mine, theirs):
    if to_owner:
        return refs[n].at[theirs], outs[n].at[:, mine]
    return refs[n].at[:, theirs], outs[n].at[mine]


def rows_start(T, t, rc, refs, outs, to_owner, rs, rr, rl):
    for n in range(len(refs)):
        for p in range(1, T):
            src, dst = row_views(refs, outs, to_owner, n, t, t ^ p)
            rc(src, dst, rs.at[n, p], rr.at[n, p], tensor=t ^ p).start()
        src, dst = row_views(refs, outs, to_owner, n, t, t)
        pltpu.make_async_copy(src, dst, rl.at[n]).start()


def rows_wait(T, t, rc, refs, outs, to_owner, rs, rr, rl):
    for n in range(len(refs)):
        for p in range(1, T):
            src, _ = row_views(refs, outs, to_owner, n, t, t ^ p)
            _, dst = row_views(refs, outs, to_owner, n, t ^ p, t)
            c = rc(src, dst, rs.at[n, p], rr.at[n, p], tensor=t ^ p)
            c.wait_send()
            c.wait_recv()
        src, dst = row_views(refs, outs, to_owner, n, t, t)
        pltpu.make_async_copy(src, dst, rl.at[n]).wait()


def gather_kernel(F, T, K, KS, w_ref, s_ref, a_ref, b_ref, W_ref, S_ref, ao_ref, bo_ref, loc_sem, zs, zr, ys, yr, xs, xr, cs, cr, ss, sr, rs, rr, rl):
    r, f, t = lax.axis_index("rep"), lax.axis_index("frame"), lax.axis_index("tensor")
    rows = w_ref.shape[1]
    half = rows // 2
    core, ypart, xpart = t ^ 1, t ^ 2, r ^ 1
    mine = pl.ds(pl.multiple_of((r % 2) * half, half), half)
    other = pl.ds(pl.multiple_of((1 - r % 2) * half, half), half)

    def rc(src, dst, ssem, rsem, **dev):
        return pltpu.make_async_remote_copy(src, dst, ssem, rsem, device_id=dev, device_id_type=MESH)

    bar = pltpu.get_barrier_semaphore()
    for d in range(1, F):
        for peer in (f - d, f + d):
            @pl.when((peer >= 0) & (peer < F))
            def _():
                pl.semaphore_signal(bar, inc=1, device_id={"frame": peer}, device_id_type=MESH)
    pl.semaphore_signal(bar, inc=1, device_id={"tensor": core}, device_id_type=MESH)
    pl.semaphore_signal(bar, inc=1, device_id={"tensor": ypart}, device_id_type=MESH)
    pl.semaphore_signal(bar, inc=1, device_id={"tensor": t ^ 3}, device_id_type=MESH)
    pl.semaphore_signal(bar, inc=1, device_id={"rep": xpart}, device_id_type=MESH)
    pl.semaphore_wait(bar, F + 3)

    def blk(k, tt, src, part=None):
        return W_ref.at[k, tt, src] if part is None else W_ref.at[k, tt, src, part]

    def zpart(k):
        return None if k < KS else mine

    def z_copy(k, src, to):
        ref = blk(k, t, src, zpart(k))
        return rc(ref, ref, zs.at[k, src, jnp.where(to > f, 1, 0)], zr.at[k, src], frame=to)

    def z_own(k, to):
        s = w_ref.at[k] if k < KS else w_ref.at[k, mine]
        return rc(s, blk(k, t, f, zpart(k)), zs.at[k, f, jnp.where(to > f, 1, 0)], zr.at[k, f], frame=to)

    def y_copy(k, src, own):
        s = w_ref.at[k, mine] if own else W_ref.at[k, t, src, mine]
        return rc(s, W_ref.at[k, t, src, mine], ys.at[k, src], yr.at[k, src], tensor=ypart)

    def y_in(k, src):
        ref = W_ref.at[k, ypart, src, mine]
        return rc(ref, ref, ys.at[k, src], yr.at[k, src], tensor=ypart)

    def x_copy(k, src, part):
        ref = W_ref.at[k, ypart, src, part]
        return rc(ref, ref, xs.at[k, src], xr.at[k, src], rep=xpart)

    def xo_copy(k, src, part):
        ref = W_ref.at[k, t, src, part]
        return rc(ref, ref, xs.at[K + k, src], xr.at[K + k, src], rep=xpart)

    def c_copy(j, k, src, tt, own=False):
        if j >= 3:
            dst = W_ref.at[k, tt, src, mine if j == 3 else other]
            return rc(dst, dst, cs.at[j, k, src], cr.at[j, k, src], tensor=core)
        if j == 0:
            dst = W_ref.at[k, tt, src]
            return rc(w_ref.at[k] if own else dst, dst, cs.at[0, k, src], cr.at[0, k, src], tensor=core)
        part = mine if j == 1 else other
        dst = W_ref.at[k, tt, src, part]
        return rc(dst, dst, cs.at[j, k, src], cr.at[j, k, src], tensor=core)

    def small(i, dst, src, **dev):
        return rc(src, dst, ss.at[i], sr.at[i], **dev)

    def each(d, fn):
        if d == 0:
            fn(f, 0)
        else:
            for sign in (-1, 1):
                src = f + sign * d
                @pl.when((src >= 0) & (src < F))
                def _():
                    fn(src, sign)

    for k in range(K):
        for to in (f - 1, f + 1):
            @pl.when((to >= 0) & (to < F))
            def _():
                z_own(k, to).start()
        y_copy(k, f, True).start()
    for k in range(K):
        c_copy(0, k, f, t, own=True).start()
        pltpu.make_async_copy(w_ref.at[k], W_ref.at[k, t, f], loc_sem.at[k]).start()
    for d in range(1, F):
        for sign in (-1, 1):
            to = f + sign * d
            @pl.when((to >= 0) & (to < F))
            def _():
                rc(s_ref, S_ref.at[t, f], ss.at[to], sr.at[f], frame=to).start()
    pltpu.make_async_copy(s_ref, S_ref.at[t, f], loc_sem.at[K]).start()
    pltpu.make_async_copy(s_ref, S_ref.at[t, f], loc_sem.at[K]).wait()

    def z_step(k, d):
        def fn(src, sign):
            z_copy(k, src, f).wait_recv()
            to = f - sign
            @pl.when((to >= 0) & (to < F))
            def _():
                z_copy(k, src, to).start()
            y_copy(k, src, False).start()
            if k < KS:
                c_copy(0, k, src, t).start()
            else:
                xo_copy(k, src, mine).start()
                c_copy(3, k, src, t).start()
        each(d, fn)

    def y_step(k, d):
        def fn(src, sign):
            y_in(k, src).wait_recv()
            x_copy(k, src, mine).start()
            c_copy(1, k, src, ypart).start()
        each(d, fn)

    def x_step(k, d):
        def fn(src, sign):
            x_copy(k, src, other).wait_recv()
            c_copy(2, k, src, ypart).start()
            if k >= KS and sign != 0:
                xo_copy(k, src, other).wait_recv()
                c_copy(4, k, src, t).start()
        each(d, fn)

    for d in range(F):
        for k in range(K):
            if d > 0:
                z_step(k, d)
            y_step(k, d)
            if d > 0:
                x_step(k, d - 1)
        if d == 1:
            rows_start(T, t, rc, (a_ref, b_ref), (ao_ref, bo_ref), True, rs, rr, rl)
            for dd in range(1, F):
                def fn(src, sign):
                    rc(s_ref, S_ref.at[t, src], ss.at[src], sr.at[src], frame=f).wait_recv()
                each(dd, fn)
            rc(S_ref.at[t], S_ref.at[t], ss.at[F], sr.at[F], tensor=ypart).start()
        if d == 2:
            rc(S_ref.at[ypart], S_ref.at[ypart], ss.at[F], sr.at[F], tensor=ypart).wait_recv()
            rc(S_ref.at[t], S_ref.at[t], ss.at[F + 1], sr.at[F + 1], tensor=core).start()
            rc(S_ref.at[ypart], S_ref.at[ypart], ss.at[F + 2], sr.at[F + 2], tensor=core).start()
    for k in range(K):
        x_step(k, F - 1)
    rows_wait(T, t, rc, (a_ref, b_ref), (ao_ref, bo_ref), True, rs, rr, rl)
    ct, cy = core, core ^ 2
    for k in range(K):
        pltpu.make_async_copy(w_ref.at[k], W_ref.at[k, t, f], loc_sem.at[k]).wait()
        for d in range(F):
            def fn(src, sign):
                if k < KS or sign == 0:
                    c_copy(0, k, src, ct).wait_recv()
                    c_copy(0, k, src, t).wait_send()
                else:
                    for j in (3, 4):
                        c_copy(j, k, src, ct).wait_recv()
                        c_copy(j, k, src, t).wait_send()
                    xo_copy(k, src, mine).wait_send()
                c_copy(1, k, src, cy).wait_recv()
                c_copy(2, k, src, cy).wait_recv()
                c_copy(1, k, src, ypart).wait_send()
                c_copy(2, k, src, ypart).wait_send()
                y_copy(k, src, False).wait_send()
                x_copy(k, src, mine).wait_send()
                if sign == 0:
                    for to in (f - 1, f + 1):
                        @pl.when((to >= 0) & (to < F))
                        def _():
                            z_own(k, to).wait_send()
                else:
                    to = f - sign
                    @pl.when((to >= 0) & (to < F))
                    def _():
                        z_copy(k, src, to).wait_send()
            each(d, fn)
    for dd in range(1, F):
        def fn(src, sign):
            rc(s_ref, S_ref.at[t, f], ss.at[src], sr.at[f], frame=src).wait_send()
        each(dd, fn)
    rc(S_ref.at[t], S_ref.at[t], ss.at[F], sr.at[F], tensor=ypart).wait_send()
    rc(S_ref.at[t], S_ref.at[t], ss.at[F + 1], sr.at[F + 1], tensor=core).wait_send()
    rc(S_ref.at[ypart], S_ref.at[ypart], ss.at[F + 2], sr.at[F + 2], tensor=core).wait_send()
    rc(S_ref.at[ct], S_ref.at[ct], ss.at[F + 1], sr.at[F + 1], tensor=core).wait_recv()
    rc(S_ref.at[cy], S_ref.at[cy], ss.at[F + 2], sr.at[F + 2], tensor=core).wait_recv()


def gather_all(wl, small, a, b):
    F, T = lax.axis_size("frame"), lax.axis_size("tensor")
    K, rows, D = wl.shape
    dma = pltpu.SemaphoreType.DMA
    any_spec = pl.BlockSpec(memory_space=pl.ANY)
    owned = (a.shape[1], a.shape[0]) + a.shape[2:]
    sds = jax.ShapeDtypeStruct
    return pl.pallas_call(
        partial(gather_kernel, F, T, K, KS),
        out_shape=(
            sds((K, T, F, rows, D), wl.dtype), sds((T, F) + small.shape, small.dtype),
            sds(owned, a.dtype), sds(owned, b.dtype),
        ),
        in_specs=[pl.BlockSpec(memory_space=pltpu.VMEM)] * 4,
        out_specs=(any_spec,) * 4,
        scratch_shapes=[
            dma((K + 1,)), dma((K, F, 2)), dma((K, F)), dma((K, F)), dma((K, F)), dma((2 * K, F)), dma((2 * K, F)),
            dma((5, K, F)), dma((5, K, F)), dma((F + 3,)), dma((F + 3,)), dma((2, T)), dma((2, T)), dma((2,)),
        ],
        compiler_params=pltpu.CompilerParams(collective_id=0, has_side_effects=True, vmem_limit_bytes=16 * 1024 * 1024),
        name="gather_all",
    )(wl, small, a, b)


def reduce_kernel(F, T, G, split, *refs):
    g_refs, h_ref, s_ref, a_ref, b_ref = refs[:G], *refs[G : G + 4]
    out_ref, sout_ref, ao_ref, bo_ref = refs[G + 4 : G + 8]
    (acc, cin, xin, yin, zdn, zup, fin, sacc, scin, sxin, syin, szin,
     lsem, cs, cr, xs, xr, ys, yr, zs, zr, fs, fr_, ss, sr, rs, rr, rl, hin, hs, hr) = refs[G + 8 :]
    K = G * split
    r, f, t = lax.axis_index("rep"), lax.axis_index("frame"), lax.axis_index("tensor")
    rows = acc.shape[3]
    half = rows // 2
    core, ypart, xpart = t ^ 1, t ^ 2, r ^ 1
    mine = pl.ds(pl.multiple_of((r % 2) * half, half), half)
    other = pl.ds(pl.multiple_of((1 - r % 2) * half, half), half)

    def rc(src, dst, ssem, rsem, **dev):
        return pltpu.make_async_remote_copy(src, dst, ssem, rsem, device_id=dev, device_id_type=MESH)

    bar = pltpu.get_barrier_semaphore()
    for d in range(1, F):
        for peer in (f - d, f + d):
            @pl.when((peer >= 0) & (peer < F))
            def _():
                pl.semaphore_signal(bar, inc=1, device_id={"frame": peer}, device_id_type=MESH)
    pl.semaphore_signal(bar, inc=1, device_id={"tensor": core}, device_id_type=MESH)
    pl.semaphore_signal(bar, inc=1, device_id={"tensor": ypart}, device_id_type=MESH)
    pl.semaphore_signal(bar, inc=1, device_id={"tensor": t ^ 3}, device_id_type=MESH)
    pl.semaphore_signal(bar, inc=1, device_id={"rep": xpart}, device_id_type=MESH)
    pl.semaphore_wait(bar, F + 3)

    def source(k, tt):
        return g_refs[k // split].at[tt, :, pl.ds((k % split) * rows, rows)]

    def load(k, j):
        return pltpu.make_async_copy(source(k, t if j == 0 else ypart), acc.at[k, j], lsem.at[k, j])

    def c_copy(k, j):
        return rc(source(k, core if j == 0 else core ^ 2), cin.at[k, j], cs.at[k, j], cr.at[k, j], tensor=core)

    def x_copy(k):
        return rc(acc.at[k, 1, :, other], xin.at[k], xs.at[k], xr.at[k], rep=xpart)

    def y_copy(k):
        return rc(acc.at[k, 1, :, mine], yin.at[k], ys.at[k], yr.at[k], tensor=ypart)

    def z_copy(k, dst, down):
        buf = zdn if down else zup
        return rc(acc.at[k, 0, dst], buf.at[k, dst], zs.at[k, dst], zr.at[k, dst, 0 if down else 1],
                  frame=f - 1 if down else f + 1)

    def pair_copy():
        return rc(h_ref, hin, hs, hr, rep=xpart)

    def fin_copy(k):
        return rc(acc.at[k, 0, f], fin.at[k], fs.at[k], fr_.at[k], rep=xpart)

    def small_copy(i):
        if i == 0:
            return rc(s_ref.at[pl.ds(0, 2), 1 - t % 2], scin, ss.at[0], sr.at[0], tensor=core)
        if i == 1:
            return rc(sacc, sxin, ss.at[1], sr.at[1], rep=xpart)
        return rc(sacc.at[1 - t // 2], syin, ss.at[2], sr.at[2], tensor=ypart)

    def small_frames(fn):
        for d in range(1, F):
            for to in (f - d, f + d):
                @pl.when((to >= 0) & (to < F))
                def _():
                    fn(to)

    def small_step(i):
        if 0 < i < 4:
            small_copy(i - 1).wait()
        if i == 1:
            for yy in range(2):
                sacc[yy] = s_ref[yy, t % 2] + scin[yy]
        elif i == 2:
            sacc[...] += sxin[...]
        elif i == 3:
            syin[...] += sacc[t // 2]
            small_frames(lambda to: rc(syin.at[to], szin.at[f], ss.at[3 + to], sr.at[3 + f], frame=to).start())
        elif i == 4:
            small_frames(lambda to: rc(syin.at[to], szin.at[to], ss.at[3 + to], sr.at[3 + to], frame=to).wait())
            szin[f] = syin[f]
            out = szin[0]
            for n in range(1, F):
                out = out + szin[n]
            sout_ref[...] = out
        if i < 3:
            small_copy(i).start()

    for k in range(K):
        for j in (1, 0):
            c_copy(k, j).start()
            load(k, j).start()
    rows_start(T, t, rc, (a_ref, b_ref), (ao_ref, bo_ref), False, rs, rr, rl)

    def add(k, j):
        c_copy(k, j).wait_recv()
        load(k, j).wait()
        @pl.loop(0, F)
        def _(i):
            acc[k, j, i] = acc[k, j, i] + cin[k, j, i]

    def step_a(k):
        add(k, 1)
        x_copy(k).start()
        add(k, 0)

    def step_b(k):
        x_copy(k).wait()
        @pl.loop(0, F)
        def _(i):
            acc[k, 1, i, mine] = acc[k, 1, i, mine] + xin[k, i]
        y_copy(k).start()

    def step_c(k):
        y_copy(k).wait()
        @pl.loop(0, F)
        def _(i):
            acc[k, 0, i, mine] = acc[k, 0, i, mine] + yin[k, i]
        for dst in range(F):
            @pl.when((f == F - 1) & (dst < f))
            def _():
                z_copy(k, dst, True).start()
            up = F - 1 - dst
            @pl.when((f == 0) & (up > f))
            def _():
                z_copy(k, up, False).start()

    def take(k, dst, down):
        buf = zdn if down else zup
        rc(buf.at[k, dst], buf.at[k, dst], zs.at[k, dst], zr.at[k, dst, 0 if down else 1], frame=f).wait_recv()
        acc[k, 0, dst] = acc[k, 0, dst] + buf[k, dst]
        @pl.when(dst != f)
        def _():
            z_copy(k, dst, down).start()

    def step_d(k):
        for hop in range(1, F):
            @pl.when(f == F - 1 - hop)
            def _():
                for dst in range(F):
                    @pl.when(dst <= f)
                    def _():
                        take(k, dst, True)
            @pl.when(f == hop)
            def _():
                for up in range(F):
                    dst = F - 1 - up
                    @pl.when(dst >= f)
                    def _():
                        take(k, dst, False)
        fin_copy(k).start()

    def step_e(k):
        fin_copy(k).wait()
        part = pl.ds((k % split) * rows, rows)
        out_ref[k // split, part, :] = acc[k, 0, f].astype(F32) + fin[k].astype(F32)

    steps = (step_a, step_b, step_c, step_d, step_e)
    for s in range(K + len(steps) - 1):
        for i, fn in enumerate(steps):
            if 0 <= s - i < K:
                fn(s - i)
        if s < 5:
            small_step(s)
        if s == K - 1:
            pair_copy().start()
    pair_copy().wait()
    for i in range(h_ref.shape[0]):
        out_ref[G + i] = h_ref[i].astype(F32) + hin[i].astype(F32)
    rows_wait(T, t, rc, (a_ref, b_ref), (ao_ref, bo_ref), False, rs, rr, rl)
    for k in range(K):
        for j in (1, 0):
            c_copy(k, j).wait_send()
        for dst in range(F):
            @pl.when(dst < f)
            def _():
                z_copy(k, dst, True).wait_send()
            @pl.when(dst > f)
            def _():
                z_copy(k, dst, False).wait_send()


def reduce_all(grads, half, small, a, b):
    F, T = lax.axis_size("frame"), lax.axis_size("tensor")
    G = len(grads)
    K = G * SPLIT
    _, _, full, D = grads[0].shape
    rows = full // SPLIT
    dma = pltpu.SemaphoreType.DMA
    V = pltpu.VMEM
    sm = small.shape[2:]
    sds = jax.ShapeDtypeStruct
    any_spec, vmem = pl.BlockSpec(memory_space=pl.ANY), pl.BlockSpec(memory_space=pltpu.VMEM)
    split_rows = (a.shape[1], a.shape[0]) + a.shape[2:]
    return pl.pallas_call(
        partial(reduce_kernel, F, T, G, SPLIT),
        out_shape=(sds((G + half.shape[0], full, D), F32), sds(sm, F32), sds(split_rows, a.dtype), sds(split_rows, b.dtype)),
        in_specs=[any_spec] * G + [vmem] * 4,
        out_specs=(vmem, vmem, any_spec, any_spec),
        scratch_shapes=[
            V((K, 2, F, rows, D), BF), V((K, 2, F, rows, D), BF), V((K, F, rows // 2, D), BF), V((K, F, rows // 2, D), BF),
            V((K, F, rows, D), BF), V((K, F, rows, D), BF), V((K, rows, D), BF),
            V((2, F) + sm, F32), V((2, F) + sm, F32), V((2, F) + sm, F32), V((F,) + sm, F32), V((F,) + sm, F32),
            dma((K, 2)), dma((K, 2)), dma((K, 2)), dma((K,)), dma((K,)), dma((K,)), dma((K,)),
            dma((K, F)), dma((K, F, 2)), dma((K,)), dma((K,)), dma((3 + F,)), dma((3 + F,)),
            dma((2, T)), dma((2, T)), dma((2,)), V(half.shape, BF), dma(()), dma(()),
        ],
        compiler_params=pltpu.CompilerParams(collective_id=1, has_side_effects=True, vmem_limit_bytes=62 * 1024 * 1024),
        name="reduce_all",
    )(*grads, half, small.reshape((2, T // 2, F) + sm).astype(F32), a, b)


def swap_core(v):
    size = lax.axis_size("tensor")
    return lax.ppermute(v, "tensor", [(i, i ^ 1) for i in range(size)])


def shards(
    tokens, query_space, key_space, value_space, output_space, query_time, key_time, value_time,
    output_time, mlp_in, bias_in, mlp_out, bias_out, gain_first, shift_first, gain_second,
    shift_second, gain_third, shift_third, place_slot, cotangent,
):
    F = lax.axis_size("frame")
    T = lax.axis_size("tensor")
    clips, frames_dev, places_dev, D = tokens.shape
    width = query_space.shape[1]
    heads = width // HEAD
    hid = mlp_in.shape[1]
    rows_w = query_space.shape[0]
    fr = clips * frames_dev // T
    fp = frames_dev // fr
    R = fr * T * PAD
    f_id = lax.axis_index("frame")
    t_id = lax.axis_index("tensor")
    core = t_id % 2

    def pack(q, k, v, o):
        return jnp.concatenate((q, k, v, o.T), axis=1)

    wl = jnp.stack(
        (
            pack(query_space, key_space, value_space, output_space),
            pack(query_time, key_time, value_time, output_time),
        )
    )
    part_bin = lax.dynamic_slice(bias_in, (f_id * (hid // F),), (hid // F,)).astype(F32)
    part_bout = lax.dynamic_slice(
        bias_out, (t_id * (bias_out.shape[0] // T),), (bias_out.shape[0] // T,)
    ).astype(F32)
    small = jnp.concatenate(
        (gain_first, shift_first, gain_second, shift_second, gain_third, shift_third, part_bout, part_bin)
    )

    def lanes(flat):
        pad = -flat.shape[-1] % 1024
        flat = jnp.pad(flat, [(0, 0)] * (flat.ndim - 1) + [(0, pad)])
        return flat.reshape(flat.shape[:-1] + (-1, 128))

    def split_places(v):
        v = jnp.pad(v, ((0, 0), (0, 0), (0, PAD - places_dev), (0, 0)))
        return v.reshape(T, fr, PAD, D)

    W, small_all, x, cot = gather_all(wl, lanes(small), split_places(tokens), split_places(cotangent))
    FT = ("frame", "tensor")
    W, wl_mlp = lax.optimization_barrier((W, jnp.stack((mlp_in, mlp_out.T))))
    W_mlp = lax.all_gather(wl_mlp, FT, axis=0, tiled=False).reshape(F, T, 2, rows_w, D)
    W = W.reshape(2, T, F * rows_w, D)
    x, cot = x.reshape(R, D), cot.reshape(R, D)
    small_all = small_all.reshape(T, F, -1)
    nv = 7 * gain_first.shape[0]
    vec = small_all[:, :, :nv].reshape(T, F, 7, -1).transpose(2, 1, 0, 3).reshape(7, D)
    vec = jnp.concatenate((vec, jnp.zeros((1, D), F32)), axis=0)
    bin_all = small_all[:, :, nv : nv + hid // F].reshape(T, hid)

    keep = place_slot >= 0
    bias = jnp.where(keep, 0.0, -1e30).astype(F32).reshape(T, places_dev)
    bias = jnp.pad(bias, ((0, 0), (0, PAD - places_dev)), constant_values=-1e30).reshape(1, T * PAD)
    rows = T * PAD

    qkv_s, os_s, xs, ht = call(
        partial(space_forward, width, heads, fr, rows),
        T,
        (x, vec, bias, W),
        [whole((R, D)), whole((8, D)), whole((1, rows)), pl.BlockSpec((1, 1, D, D), lambda t: (0, t, 0, 0))],
        [((T, R, 3 * width), BF), ((T, R, width), BF), ((R, D), F32), ((R, D), BF)],
        [
            pl.BlockSpec((1, R, 3 * width), lambda t: (t, 0, 0)),
            pl.BlockSpec((1, R, width), lambda t: (t, 0, 0)),
            whole((R, D)),
            whole((R, D)),
        ],
        [pltpu.VMEM((R, D), BF)],
        name="space_forward",
    )

    groups = PAD // 8
    nf = 2 * F * fr
    size = nf * 8
    RT = groups * size

    def to_time(own):
        v = own.transpose(1, 0, 2, 3)
        return lax.all_to_all(v, "frame", split_axis=0, concat_axis=0, tiled=True)

    def group_rows(a, b):
        v = jnp.stack((a, b)).reshape(nf, groups, 8, a.shape[-1])
        return v.transpose(1, 0, 2, 3).reshape(RT, a.shape[-1])

    def ungroup_rows(v):
        n = v.shape[-1]
        return v.reshape(groups, nf, 8, n).transpose(1, 0, 2, 3).reshape(2, F, fr, PAD, n)

    def to_frames(v):
        v = lax.all_to_all(v, "frame", split_axis=0, concat_axis=0, tiled=True)
        return v.transpose(1, 0, 2, 3).reshape(R, v.shape[-1])

    h_own = to_time(ht.reshape(fr, T, PAD, D))
    h_t = group_rows(h_own, swap_core(h_own))
    keep_q = lax.dynamic_slice(
        jnp.pad(keep.astype(F32).reshape(T, places_dev), ((0, 0), (0, PAD - places_dev))), (f_id, 0), (1, PAD)
    )
    mask = jnp.broadcast_to(keep_q.reshape(groups, 1, 8), (groups, nf, 8)).reshape(RT, 1)
    core_arr = core.reshape(1).astype(jnp.int32)
    halves = T // 2
    time_w = pl.BlockSpec((1, 1, D, D), lambda i, c: (1, c[0] + 2 * i, 0, 0))
    per_half = lambda n: pl.BlockSpec((1, RT, n), lambda i, c: (i, 0, 0))
    qkv_t, ot = call(
        partial(time_forward, width, heads, groups, size, 8),
        halves,
        (core_arr, h_t, W, mask),
        [whole((RT, D)), time_w, whole((RT, 1))],
        [((halves, RT, 3 * width), BF), ((halves, RT, width), BF)],
        [per_half(3 * width), per_half(width)],
        [],
        prefetch=1,
        name="time_forward",
    )
    ot_u = jnp.stack([ungroup_rows(ot[i]) for i in range(halves)], axis=-2)
    ot_u = ot_u.reshape(2, F, fr, PAD, halves * width)
    ot_mine, ot_other = to_frames(ot_u[0]), to_frames(swap_core(ot_u[1]))

    def by_tensor(mine, other):
        m = mine.reshape(R, halves, width)
        o = other.reshape(R, halves, width)
        first = jnp.where(core == 0, m, o)
        second = jnp.where(core == 0, o, m)
        return jnp.stack((first, second), axis=2).reshape(R, T, width).transpose(1, 0, 2)

    ot_all = by_tensor(ot_mine, ot_other)
    win_spec = lambda kind: pl.BlockSpec((F, 1, 1, rows_w, D), lambda t: (0, t, kind, 0, 0))
    res, gt, dot_all, g_mlp, g_wt, sv_m, gb = call(
        partial(mlp_both, width, T),
        T,
        (xs, cot, ot_all, vec, bin_all, W, W_mlp, W_mlp),
        [
            whole((R, D)), whole((R, D)), whole((T, R, width)), whole((8, D)), whole((T, hid)),
            pl.BlockSpec((1, T, D, D), lambda t: (1, 0, 0, 0)), win_spec(0), win_spec(1),
        ],
        [
            ((R, D), BF), ((R, D), F32), ((T, R, width), BF), ((F, T, 2, rows_w, D), BF),
            ((T, D, width), BF), ((8, D), F32), ((T, hid), F32),
        ],
        [
            whole((R, D)), whole((R, D)), whole((T, R, width)),
            pl.BlockSpec((F, 1, 2, rows_w, D), lambda t: (0, t, 0, 0, 0)),
            whole((T, D, width)), whole((8, D)), whole((T, hid)),
        ],
        [pltpu.VMEM((R, D), F32), pltpu.VMEM((R, D), BF), pltpu.VMEM((R, D), F32), pltpu.VMEM((R, D), F32)],
        name="mlp_both",
    )
    share_mlp = lax.psum_scatter(
        g_mlp.reshape(F * T, 2, rows_w, D), FT, scatter_dimension=0, tiled=False
    )
    d = dot_all.reshape(halves, 2, R, width)
    d_mine = jnp.where(core == 0, d[:, 0], d[:, 1])
    d_other = jnp.where(core == 0, d[:, 1], d[:, 0])
    as_frames = lambda v: v.transpose(1, 0, 2).reshape(fr, T, PAD, halves * width)
    d_own = to_time(as_frames(d_mine))
    d_par = to_time(swap_core(as_frames(d_other)))
    d_t = group_rows(d_own, d_par).reshape(RT, halves, width).transpose(1, 0, 2)
    g_time, dh_part = call(
        partial(time_backward, width, heads, groups, size, 8),
        halves,
        (core_arr, h_t, W, mask, qkv_t, d_t),
        [whole((RT, D)), time_w, whole((RT, 1)), per_half(3 * width), per_half(width)],
        [((halves, D, 3 * width), BF), ((RT, D), F32)],
        [pl.BlockSpec((1, D, 3 * width), lambda i, c: (i, 0, 0)), whole((RT, D))],
        [pltpu.VMEM((RT, 3 * width), BF)],
        prefetch=1,
        name="time_backward",
    )
    dh_u = ungroup_rows(dh_part)
    dh_sum = (dh_u[0] + swap_core(dh_u[1].astype(BF)).astype(F32)).astype(BF)
    dht = to_frames(dh_sum)

    gx, g_space, sv_s = call(
        partial(space_backward, width, heads, fr, rows),
        T,
        (x, xs, gt, dht, vec, bias, W, qkv_s, os_s),
        [
            whole((R, D)), whole((R, D)), whole((R, D)), whole((R, D)), whole((8, D)), whole((1, rows)),
            pl.BlockSpec((1, 1, D, D), lambda t: (0, t, 0, 0)),
            pl.BlockSpec((1, R, 3 * width), lambda t: (t, 0, 0)),
            pl.BlockSpec((1, R, width), lambda t: (t, 0, 0)),
        ],
        [((R, D), BF), ((T, D, D), BF), ((8, D), F32)],
        [whole((R, D)), pl.BlockSpec((1, D, D), lambda t: (t, 0, 0)), whole((8, D))],
        [
            pltpu.VMEM((R, D), BF), pltpu.VMEM((R, D), F32), pltpu.VMEM((R, D), BF), pltpu.VMEM((R, D), F32),
            pltpu.VMEM((R, 3 * width), BF),
        ],
        name="space_backward",
    )
    zero = jnp.zeros_like(g_time)
    g_first = jnp.where(core == 0, g_time, zero)
    g_second = jnp.where(core == 0, zero, g_time)
    g_qkv = jnp.stack((g_first, g_second), axis=1).reshape(T, D, 3 * width)
    kinds = (g_space, jnp.concatenate((g_qkv, g_wt), axis=2))
    kinds = tuple(g.reshape(T, F, rows_w, D) for g in kinds)
    n = gain_first.shape[0]
    nb = bias_out.shape[0]
    norms = jnp.concatenate((sv_s[0:4], sv_m[0:2]), axis=0).reshape(6, F, T, n).transpose(2, 1, 0, 3)
    small_g = jnp.concatenate(
        (
            norms.reshape(T, F, 6 * n),
            jnp.broadcast_to(sv_m[2].reshape(1, F, nb), (T, F, nb)),
            jnp.broadcast_to(gb[:, None, :], (T, F, hid)),
        ),
        axis=2,
    )
    share, smalls, res_rows, gx_rows = reduce_all(
        kinds, share_mlp, lanes(small_g), res.reshape(fr, T, PAD, D), gx.reshape(fr, T, PAD, D)
    )
    reps = lax.axis_size("rep")
    if reps > 2:
        share, smalls = (lax.psum(0.5 * v, "rep") for v in (share, smalls))
    smalls = smalls.reshape(-1)

    def join_places(v):
        return v.reshape(clips, frames_dev, PAD, D)[:, :, :places_dev]

    def unpack(g):
        return g[:, :width], g[:, width : 2 * width], g[:, 2 * width : 3 * width], g[:, 3 * width :].T

    gs_q, gs_k, gs_v, gs_o = unpack(share[0])
    gt_q, gt_k, gt_v, gt_o = unpack(share[1])
    own = lambda i: smalls[i * n : (i + 1) * n]
    return (
        join_places(res_rows),
        join_places(gx_rows).astype(F32),
        gs_q, gs_k, gs_v, gs_o,
        gt_q, gt_k, gt_v, gt_o,
        share[2],
        smalls[6 * n + nb : 6 * n + nb + hid],
        share[3].T,
        smalls[6 * n : 6 * n + nb],
        own(0), own(1), own(2), own(3), own(4), own(5),
    )


def solution(mesh):
    rows = P("rep", "frame", "tensor", None)
    ft, tf, vec = P("frame", "tensor"), P("tensor", "frame"), P(("frame", "tensor"))
    placed = (
        rows, ft, ft, ft, tf, ft, ft, ft, tf, ft, P("tensor"), tf, P("frame"),
        vec, vec, vec, vec, vec, vec, P(), rows,
    )
    return jax.shard_map(
        shards,
        mesh=mesh,
        in_specs=placed,
        out_specs=(
            rows, rows, ft, ft, ft, tf, ft, ft, ft, tf, ft, P("tensor"), tf, P("frame"),
            vec, vec, vec, vec, vec, vec,
        ),
        check_vma=False,
    )
```

```python
from functools import partial

import jax
import jax.numpy as jnp
from jax import lax
from jax.experimental import pallas as pl
from jax.experimental.pallas import tpu as pltpu
from jax.sharding import PartitionSpec as P

HEAD = 64
PAD = 56
BF = jnp.bfloat16
F32 = jnp.float32
NT = (((1,), (1,)), ((), ()))
TN = (((0,), (0,)), ((), ()))
GELU_C = 0.7978845608028654
SCALE = HEAD ** (-0.5)
MESH = pl.DeviceIdType.MESH
KS = 1
SPLIT = 2


def dot(a, b, dims=(((1,), (0,)), ((), ()))):
    return lax.dot_general(a, b, dims, preferred_element_type=F32)


def norm_stats(v):
    m = jnp.mean(v, axis=-1, keepdims=True)
    off = v - m
    s = jnp.mean(off * off, axis=-1, keepdims=True)
    r = lax.rsqrt(s + 1e-06)
    return off * r, r


def norm(v, g, b):
    xhat, _ = norm_stats(v)
    return xhat * g + b


def norm_back(v, g, dy):
    xhat, r = norm_stats(v)
    dyg = dy * g
    mean1 = jnp.mean(dyg, axis=-1, keepdims=True)
    mean2 = jnp.mean(dyg * xhat, axis=-1, keepdims=True)
    dx = r * (dyg - mean1 - xhat * mean2)
    dgain = jnp.sum(dy * xhat, axis=0, keepdims=True)
    dshift = jnp.sum(dy, axis=0, keepdims=True)
    return dx, dgain, dshift


def softmax(s):
    m = jnp.max(s, axis=-1, keepdims=True)
    e = jnp.exp(s - m)
    return e / jnp.sum(e, axis=-1, keepdims=True)


def attend_head(q, k, v, bias):
    s = dot(q, k, NT) * SCALE + bias
    p = softmax(s)
    return dot(p.astype(BF), v).astype(BF)


def attend_head_back(do, q, k, v, bias):
    s = dot(q, k, NT) * SCALE + bias
    p = softmax(s)
    dp = dot(do, v, NT)
    dv = dot(p.astype(BF), do, TN)
    inner = jnp.sum(dp * p, axis=-1, keepdims=True)
    ds = (p * (dp - inner)).astype(BF)
    dq = dot(ds, k) * SCALE
    dk = dot(ds, q, TN) * SCALE
    return dq.astype(BF), dk.astype(BF), dv.astype(BF)


def space_forward(width, heads, frames, rows, x_ref, vec_ref, bias_ref, w_ref, qkv_ref, os_ref, xs_ref, ht_ref, h_scr):
    t = pl.program_id(0)

    @pl.when(t == 0)
    def _():
        x = x_ref[...].astype(F32)
        h_scr[...] = norm(x, vec_ref[0:1, :], vec_ref[1:2, :]).astype(BF)
        xs_ref[...] = x

    qkv_ref[0] = dot(h_scr[...], w_ref[0, 0, :, : 3 * width]).astype(BF)
    bias = bias_ref[...]
    for i in range(frames):
        r = pl.ds(i * rows, rows)
        for h in range(heads):
            q = qkv_ref[0, r, h * HEAD : (h + 1) * HEAD]
            k = qkv_ref[0, r, width + h * HEAD : width + (h + 1) * HEAD]
            v = qkv_ref[0, r, 2 * width + h * HEAD : 2 * width + (h + 1) * HEAD]
            os_ref[0, r, h * HEAD : (h + 1) * HEAD] = attend_head(q, k, v, bias)
    xs_ref[...] += dot(os_ref[0], w_ref[0, 0, :, 3 * width :], NT)

    @pl.when(t == pl.num_programs(0) - 1)
    def _():
        ht_ref[...] = norm(xs_ref[...], vec_ref[2:3, :], vec_ref[3:4, :]).astype(BF)


def space_backward(
    width, heads, frames, rows,
    x_ref, xs_ref, gt_ref, dht_ref, vec_ref, bias_ref, w_ref, qkv_ref, os_ref,
    gx_ref, gw_ref, sv_ref, h_scr, gs_scr, dat_scr, dh_scr, dqkv_scr, dos_scr,
):
    t = pl.program_id(0)

    @pl.when(t == 0)
    def _():
        x = x_ref[...].astype(F32)
        h_scr[...] = norm(x, vec_ref[0:1, :], vec_ref[1:2, :]).astype(BF)
        dx, dg, db = norm_back(xs_ref[...], vec_ref[2:3, :], dht_ref[...].astype(F32))
        gs = gt_ref[...] + dx
        gs_scr[...] = gs
        dat_scr[...] = gs.astype(BF)
        sv_ref[2:3, :] = dg
        sv_ref[3:4, :] = db
        sv_ref[4:8, :] = jnp.zeros((4, sv_ref.shape[1]), F32)
        dh_scr[...] = jnp.zeros_like(dh_scr)

    dat = dat_scr[...]
    dos_scr[...] = dot(dat, w_ref[0, 0, :, 3 * width :]).astype(BF)
    bias = bias_ref[...]

    def frame(i, carry):
        r = pl.ds(pl.multiple_of(i * rows, 32), rows)
        for h in range(heads):
            a, b, c = (slice(j * width + h * HEAD, j * width + (h + 1) * HEAD) for j in range(3))
            dq, dk, dv = attend_head_back(
                dos_scr[r, a], qkv_ref[0, r, a], qkv_ref[0, r, b], qkv_ref[0, r, c], bias
            )
            dqkv_scr[r, a] = dq
            dqkv_scr[r, b] = dk
            dqkv_scr[r, c] = dv
        return carry

    lax.fori_loop(0, frames, frame, 0)
    dqkv = dqkv_scr[...]
    gw_ref[0, :, : 3 * width] = dot(h_scr[...], dqkv, TN).astype(BF)
    gw_ref[0, :, 3 * width :] = dot(dat, os_ref[0], TN).astype(BF)
    dh_scr[...] += dot(dqkv, w_ref[0, 0, :, : 3 * width], NT)

    @pl.when(t == pl.num_programs(0) - 1)
    def _():
        dx, dg, db = norm_back(x_ref[...].astype(F32), vec_ref[0:1, :], dh_scr[...])
        gx_ref[...] = (gs_scr[...] + dx).astype(gx_ref.dtype)
        sv_ref[0:1, :] = dg
        sv_ref[1:2, :] = db


def group_bias(size, places):
    i = lax.broadcasted_iota(jnp.int32, (size, size), 0)
    j = lax.broadcasted_iota(jnp.int32, (size, size), 1)
    return jnp.where(i % places == j % places, 0.0, -1e30).astype(F32)


def time_forward(width, heads, groups, size, places, core_ref, h_ref, w_ref, mask_ref, qkv_ref, ot_ref):
    qkv_ref[0] = dot(h_ref[...], w_ref[0, 0, :, : 3 * width]).astype(BF)
    bias = group_bias(size, places)

    def one(g, carry):
        r = pl.ds(pl.multiple_of(g * size, size), size)
        keep = mask_ref[r, :]
        for h in range(heads):
            a, b, c = (slice(j * width + h * HEAD, j * width + (h + 1) * HEAD) for j in range(3))
            s = dot(qkv_ref[0, r, a], qkv_ref[0, r, b], NT) * SCALE + bias
            o = dot(softmax(s).astype(BF), qkv_ref[0, r, c])
            ot_ref[0, r, a] = jnp.where(keep > 0, o, 0.0).astype(BF)
        return carry

    lax.fori_loop(0, groups, one, 0)


def time_backward(
    width, heads, groups, size, places,
    core_ref, h_ref, w_ref, mask_ref, qkv_ref, do_ref, gwt_ref, gw_ref, dh_ref, dqkv_scr,
):
    t = pl.program_id(0)
    part = gw_ref.shape[1] // 8

    def carry_over(i, carry):
        r = pl.ds(pl.multiple_of(i * part, part), part)
        gw_ref[0, r, 3 * width :] = gwt_ref[0, r]
        return carry

    lax.fori_loop(0, 8, carry_over, 0)

    @pl.when(t % 2 != core_ref[0])
    def _():
        def clear(i, carry):
            r = pl.ds(pl.multiple_of(i * part, part), part)
            gw_ref[0, r, : 3 * width] = jnp.zeros((part, 3 * width), BF)
            return carry

        lax.fori_loop(0, 8, clear, 0)

    @pl.when(t % 2 == core_ref[0])
    def _():
        bias = group_bias(size, places)

        def one(g, carry):
            r = pl.ds(pl.multiple_of(g * size, size), size)
            keep = mask_ref[r, :]
            for h in range(heads):
                a, b, c = (slice(j * width + h * HEAD, j * width + (h + 1) * HEAD) for j in range(3))
                do = jnp.where(keep > 0, do_ref[0, r, a].astype(F32), 0.0).astype(BF)
                dq, dk, dv = attend_head_back(do, qkv_ref[0, r, a], qkv_ref[0, r, b], qkv_ref[0, r, c], bias)
                dqkv_scr[r, a] = dq
                dqkv_scr[r, b] = dk
                dqkv_scr[r, c] = dv
            return carry

        lax.fori_loop(0, groups, one, 0)
        dqkv = dqkv_scr[...]
        gw_ref[0, :, : 3 * width] = dot(h_ref[...], dqkv, TN).astype(BF)
        dh = dot(dqkv, w_ref[0, 0, :, : 3 * width], NT)

        dh_ref[...] = dh + jnp.where(t < 2, 0.0, dh_ref[...])


def mlp_both(
    width, halves,
    core_ref, xs_ref, cot_ref, ot_ref, vec_ref, bin_ref, wt_ref, win_ref, wout_ref,
    res_ref, gt_ref, do_ref, gg_ref, gwt_ref, sv_ref, gb_ref,
    xt_scr, hm_scr, xm_scr, dhm_scr,
):
    t = pl.program_id(0)

    def each_core(fn):
        lax.fori_loop(0, 2, lambda c, carry: fn(c, jnp.where(c == core_ref[0], 0, 1)) or carry, 0)

    @pl.when(t == 0)
    def _():
        xt_scr[...] = xs_ref[...]

        def add(c, rel):
            for i in range(halves):
                cols = slice(i * width, (i + 1) * width)
                xt_scr[...] += dot(ot_ref[rel, :, cols], wt_ref[0, 2 * i + c, :, 3 * width :], NT)

        each_core(add)
        xt = xt_scr[...]
        hm_scr[...] = norm(xt, vec_ref[4:5, :], vec_ref[5:6, :]).astype(BF)
        xm_scr[...] = xt + vec_ref[6:7, :]
        dhm_scr[...] = jnp.zeros_like(dhm_scr)

    hm = hm_scr[...]
    dz = cot_ref[...]
    lines, _, _, rows, cols = win_ref.shape
    win = win_ref[:, 0, 0].reshape(lines * rows, cols)
    wout = wout_ref[:, 0, 0].reshape(lines * rows, cols)
    pre = dot(hm, win) + bin_ref[pl.ds(t, 1), :]
    sq = pre * pre
    th = jnp.tanh(GELU_C * (pre + 0.044715 * (pre * sq)))
    hidden = (0.5 * pre * (1.0 + th)).astype(BF)
    xm_scr[...] += dot(hidden, wout, NT)
    slope = 0.5 * (1.0 + th) + 0.5 * pre * (1.0 - th * th) * (GELU_C * (1.0 + 0.134145 * sq))
    dpre = dot(dz, wout) * slope
    dpre_b = dpre.astype(BF)
    gb_ref[pl.ds(t, 1), :] = jnp.sum(dpre_b.astype(F32), axis=0, keepdims=True)
    gg_ref[:, 0, 0] = dot(hm, dpre_b, TN).astype(BF).reshape(lines, rows, cols)
    gg_ref[:, 0, 1] = dot(dz, hidden, TN).astype(BF).reshape(lines, rows, cols)
    dhm_scr[...] += dot(dpre_b, win, NT)

    @pl.when(t == pl.num_programs(0) - 1)
    def _():
        res_ref[...] = xm_scr[...].astype(BF)
        gm = dz.astype(F32)
        dx, dg, db = norm_back(xt_scr[...], vec_ref[4:5, :], dhm_scr[...])
        gt = gm + dx
        gt_ref[...] = gt
        dat = gt.astype(BF)

        def back(c, rel):
            for i in range(halves):
                cols = slice(i * width, (i + 1) * width)
                do_ref[rel, :, cols] = dot(dat, wt_ref[0, 2 * i + c, :, 3 * width :]).astype(BF)
                gwt_ref[2 * i + c] = dot(dat, ot_ref[rel, :, cols], TN).astype(BF)

        each_core(back)
        sv_ref[...] = jnp.zeros_like(sv_ref)
        sv_ref[0:1, :] = dg
        sv_ref[1:2, :] = db
        sv_ref[2:3, :] = jnp.sum(gm, axis=0, keepdims=True)


def whole(shape):
    zero = (0,) * len(shape)
    return pl.BlockSpec(shape, lambda *_: zero)


def call(body, grid, ins, in_specs, outs, out_specs, scratch, prefetch=0, name=None):
    return pl.pallas_call(
        body,
        out_shape=tuple(jax.ShapeDtypeStruct(s, d) for s, d in outs),
        grid_spec=pltpu.PrefetchScalarGridSpec(
            num_scalar_prefetch=prefetch,
            grid=(grid,),
            in_specs=in_specs,
            out_specs=tuple(out_specs),
            scratch_shapes=scratch,
        ),
        compiler_params=pltpu.CompilerParams(
            dimension_semantics=("arbitrary",), vmem_limit_bytes=60 * 1024 * 1024
        ),
        name=name,
    )(*ins)


def row_views(refs, outs, to_owner, n, mine, theirs):
    if to_owner:
        return refs[n].at[theirs], outs[n].at[:, mine]
    return refs[n].at[:, theirs], outs[n].at[mine]


def rows_start(T, t, rc, refs, outs, to_owner, rs, rr, rl):
    for n in range(len(refs)):
        for p in range(1, T):
            src, dst = row_views(refs, outs, to_owner, n, t, t ^ p)
            rc(src, dst, rs.at[n, p], rr.at[n, p], tensor=t ^ p).start()
        src, dst = row_views(refs, outs, to_owner, n, t, t)
        pltpu.make_async_copy(src, dst, rl.at[n]).start()


def rows_wait(T, t, rc, refs, outs, to_owner, rs, rr, rl):
    for n in range(len(refs)):
        for p in range(1, T):
            src, _ = row_views(refs, outs, to_owner, n, t, t ^ p)
            _, dst = row_views(refs, outs, to_owner, n, t ^ p, t)
            c = rc(src, dst, rs.at[n, p], rr.at[n, p], tensor=t ^ p)
            c.wait_send()
            c.wait_recv()
        src, dst = row_views(refs, outs, to_owner, n, t, t)
        pltpu.make_async_copy(src, dst, rl.at[n]).wait()


def gather_kernel(F, T, K, KS, w_ref, s_ref, a_ref, W_ref, S_ref, ao_ref, loc_sem, zs, zr, ys, yr, xs, xr, cs, cr, ss, sr, rs, rr, rl):
    r, f, t = lax.axis_index("rep"), lax.axis_index("frame"), lax.axis_index("tensor")
    rows = w_ref.shape[1]
    half = rows // 2
    core, ypart, xpart = t ^ 1, t ^ 2, r ^ 1
    mine = pl.ds(pl.multiple_of((r % 2) * half, half), half)
    other = pl.ds(pl.multiple_of((1 - r % 2) * half, half), half)

    def rc(src, dst, ssem, rsem, **dev):
        return pltpu.make_async_remote_copy(src, dst, ssem, rsem, device_id=dev, device_id_type=MESH)

    bar = pltpu.get_barrier_semaphore()
    for d in range(1, F):
        for peer in (f - d, f + d):
            @pl.when((peer >= 0) & (peer < F))
            def _():
                pl.semaphore_signal(bar, inc=1, device_id={"frame": peer}, device_id_type=MESH)
    pl.semaphore_signal(bar, inc=1, device_id={"tensor": core}, device_id_type=MESH)
    pl.semaphore_signal(bar, inc=1, device_id={"tensor": ypart}, device_id_type=MESH)
    pl.semaphore_signal(bar, inc=1, device_id={"tensor": t ^ 3}, device_id_type=MESH)
    pl.semaphore_signal(bar, inc=1, device_id={"rep": xpart}, device_id_type=MESH)
    pl.semaphore_wait(bar, F + 3)

    def blk(k, tt, src, part=None):
        return W_ref.at[k, tt, src] if part is None else W_ref.at[k, tt, src, part]

    def zpart(k):
        return None if k < KS else mine

    def z_copy(k, src, to):
        ref = blk(k, t, src, zpart(k))
        return rc(ref, ref, zs.at[k, src, jnp.where(to > f, 1, 0)], zr.at[k, src], frame=to)

    def z_own(k, to):
        s = w_ref.at[k] if k < KS else w_ref.at[k, mine]
        return rc(s, blk(k, t, f, zpart(k)), zs.at[k, f, jnp.where(to > f, 1, 0)], zr.at[k, f], frame=to)

    def y_copy(k, src, own):
        s = w_ref.at[k, mine] if own else W_ref.at[k, t, src, mine]
        return rc(s, W_ref.at[k, t, src, mine], ys.at[k, src], yr.at[k, src], tensor=ypart)

    def y_in(k, src):
        ref = W_ref.at[k, ypart, src, mine]
        return rc(ref, ref, ys.at[k, src], yr.at[k, src], tensor=ypart)

    def x_copy(k, src, part):
        ref = W_ref.at[k, ypart, src, part]
        return rc(ref, ref, xs.at[k, src], xr.at[k, src], rep=xpart)

    def xo_copy(k, src, part):
        ref = W_ref.at[k, t, src, part]
        return rc(ref, ref, xs.at[K + k, src], xr.at[K + k, src], rep=xpart)

    def c_copy(j, k, src, tt, own=False):
        if j >= 3:
            dst = W_ref.at[k, tt, src, mine if j == 3 else other]
            return rc(dst, dst, cs.at[j, k, src], cr.at[j, k, src], tensor=core)
        if j == 0:
            dst = W_ref.at[k, tt, src]
            return rc(w_ref.at[k] if own else dst, dst, cs.at[0, k, src], cr.at[0, k, src], tensor=core)
        part = mine if j == 1 else other
        dst = W_ref.at[k, tt, src, part]
        return rc(dst, dst, cs.at[j, k, src], cr.at[j, k, src], tensor=core)

    def small(i, dst, src, **dev):
        return rc(src, dst, ss.at[i], sr.at[i], **dev)

    def each(d, fn):
        if d == 0:
            fn(f, 0)
        else:
            for sign in (-1, 1):
                src = f + sign * d
                @pl.when((src >= 0) & (src < F))
                def _():
                    fn(src, sign)

    for k in range(K):
        for to in (f - 1, f + 1):
            @pl.when((to >= 0) & (to < F))
            def _():
                z_own(k, to).start()
        y_copy(k, f, True).start()
    for k in range(K):
        c_copy(0, k, f, t, own=True).start()
        pltpu.make_async_copy(w_ref.at[k], W_ref.at[k, t, f], loc_sem.at[k]).start()
    for d in range(1, F):
        for sign in (-1, 1):
            to = f + sign * d
            @pl.when((to >= 0) & (to < F))
            def _():
                rc(s_ref, S_ref.at[t, f], ss.at[to], sr.at[f], frame=to).start()
    pltpu.make_async_copy(s_ref, S_ref.at[t, f], loc_sem.at[K]).start()
    pltpu.make_async_copy(s_ref, S_ref.at[t, f], loc_sem.at[K]).wait()

    def z_step(k, d):
        def fn(src, sign):
            z_copy(k, src, f).wait_recv()
            to = f - sign
            @pl.when((to >= 0) & (to < F))
            def _():
                z_copy(k, src, to).start()
            y_copy(k, src, False).start()
            if k < KS:
                c_copy(0, k, src, t).start()
            else:
                xo_copy(k, src, mine).start()
                c_copy(3, k, src, t).start()
        each(d, fn)

    def y_step(k, d):
        def fn(src, sign):
            y_in(k, src).wait_recv()
            x_copy(k, src, mine).start()
            c_copy(1, k, src, ypart).start()
        each(d, fn)

    def x_step(k, d):
        def fn(src, sign):
            x_copy(k, src, other).wait_recv()
            c_copy(2, k, src, ypart).start()
            if k >= KS and sign != 0:
                xo_copy(k, src, other).wait_recv()
                c_copy(4, k, src, t).start()
        each(d, fn)

    for d in range(F):
        for k in range(K):
            if d > 0:
                z_step(k, d)
            y_step(k, d)
            if d > 0:
                x_step(k, d - 1)
        if d == 1:
            rows_start(T, t, rc, (a_ref,), (ao_ref,), True, rs, rr, rl)
            for dd in range(1, F):
                def fn(src, sign):
                    rc(s_ref, S_ref.at[t, src], ss.at[src], sr.at[src], frame=f).wait_recv()
                each(dd, fn)
            rc(S_ref.at[t], S_ref.at[t], ss.at[F], sr.at[F], tensor=ypart).start()
        if d == 2:
            rc(S_ref.at[ypart], S_ref.at[ypart], ss.at[F], sr.at[F], tensor=ypart).wait_recv()
            rc(S_ref.at[t], S_ref.at[t], ss.at[F + 1], sr.at[F + 1], tensor=core).start()
            rc(S_ref.at[ypart], S_ref.at[ypart], ss.at[F + 2], sr.at[F + 2], tensor=core).start()
    for k in range(K):
        x_step(k, F - 1)
    rows_wait(T, t, rc, (a_ref,), (ao_ref,), True, rs, rr, rl)
    ct, cy = core, core ^ 2
    for k in range(K):
        pltpu.make_async_copy(w_ref.at[k], W_ref.at[k, t, f], loc_sem.at[k]).wait()
        for d in range(F):
            def fn(src, sign):
                if k < KS or sign == 0:
                    c_copy(0, k, src, ct).wait_recv()
                    c_copy(0, k, src, t).wait_send()
                else:
                    for j in (3, 4):
                        c_copy(j, k, src, ct).wait_recv()
                        c_copy(j, k, src, t).wait_send()
                    xo_copy(k, src, mine).wait_send()
                c_copy(1, k, src, cy).wait_recv()
                c_copy(2, k, src, cy).wait_recv()
                c_copy(1, k, src, ypart).wait_send()
                c_copy(2, k, src, ypart).wait_send()
                y_copy(k, src, False).wait_send()
                x_copy(k, src, mine).wait_send()
                if sign == 0:
                    for to in (f - 1, f + 1):
                        @pl.when((to >= 0) & (to < F))
                        def _():
                            z_own(k, to).wait_send()
                else:
                    to = f - sign
                    @pl.when((to >= 0) & (to < F))
                    def _():
                        z_copy(k, src, to).wait_send()
            each(d, fn)
    for dd in range(1, F):
        def fn(src, sign):
            rc(s_ref, S_ref.at[t, f], ss.at[src], sr.at[f], frame=src).wait_send()
        each(dd, fn)
    rc(S_ref.at[t], S_ref.at[t], ss.at[F], sr.at[F], tensor=ypart).wait_send()
    rc(S_ref.at[t], S_ref.at[t], ss.at[F + 1], sr.at[F + 1], tensor=core).wait_send()
    rc(S_ref.at[ypart], S_ref.at[ypart], ss.at[F + 2], sr.at[F + 2], tensor=core).wait_send()
    rc(S_ref.at[ct], S_ref.at[ct], ss.at[F + 1], sr.at[F + 1], tensor=core).wait_recv()
    rc(S_ref.at[cy], S_ref.at[cy], ss.at[F + 2], sr.at[F + 2], tensor=core).wait_recv()


def gather_all(wl, small, a):
    F, T = lax.axis_size("frame"), lax.axis_size("tensor")
    K, rows, D = wl.shape
    dma = pltpu.SemaphoreType.DMA
    hbm = pl.BlockSpec(memory_space=pltpu.HBM)
    owned = (a.shape[1], a.shape[0]) + a.shape[2:]
    sds = jax.ShapeDtypeStruct
    return pl.pallas_call(
        partial(gather_kernel, F, T, K, KS),
        out_shape=(
            sds((K, T, F, rows, D), wl.dtype), sds((T, F) + small.shape, small.dtype),
            sds(owned, a.dtype),
        ),
        in_specs=[pl.BlockSpec(memory_space=pltpu.VMEM)] * 3,
        out_specs=(hbm,) * 3,
        scratch_shapes=[
            dma((K + 1,)), dma((K, F, 2)), dma((K, F)), dma((K, F)), dma((K, F)), dma((2 * K, F)), dma((2 * K, F)),
            dma((5, K, F)), dma((5, K, F)), dma((F + 3,)), dma((F + 3,)), dma((1, T)), dma((1, T)), dma((1,)),
        ],
        compiler_params=pltpu.CompilerParams(collective_id=0, has_side_effects=True, vmem_limit_bytes=62 * 1024 * 1024),
        name="gather_all",
    )(wl, small, a)


def reduce_kernel(F, T, G, split, *refs):
    g_refs, h_ref, s_ref, a_ref = refs[:G], *refs[G : G + 3]
    out_ref, sout_ref, ao_ref = refs[G + 3 : G + 6]
    (acc, cin, xin, yin, zdn, zup, fin, sacc, scin, sxin, syin, szin,
     lsem, cs, cr, xs, xr, ys, yr, zs, zr, fs, fr_, ss, sr, rs, rr, rl, hin, hs, hr) = refs[G + 6 :]
    K = G * split
    r, f, t = lax.axis_index("rep"), lax.axis_index("frame"), lax.axis_index("tensor")
    rows = acc.shape[3]
    half = rows // 2
    core, ypart, xpart = t ^ 1, t ^ 2, r ^ 1
    mine = pl.ds(pl.multiple_of((r % 2) * half, half), half)
    other = pl.ds(pl.multiple_of((1 - r % 2) * half, half), half)

    def rc(src, dst, ssem, rsem, **dev):
        return pltpu.make_async_remote_copy(src, dst, ssem, rsem, device_id=dev, device_id_type=MESH)

    bar = pltpu.get_barrier_semaphore()
    for d in range(1, F):
        for peer in (f - d, f + d):
            @pl.when((peer >= 0) & (peer < F))
            def _():
                pl.semaphore_signal(bar, inc=1, device_id={"frame": peer}, device_id_type=MESH)
    pl.semaphore_signal(bar, inc=1, device_id={"tensor": core}, device_id_type=MESH)
    pl.semaphore_signal(bar, inc=1, device_id={"tensor": ypart}, device_id_type=MESH)
    pl.semaphore_signal(bar, inc=1, device_id={"tensor": t ^ 3}, device_id_type=MESH)
    pl.semaphore_signal(bar, inc=1, device_id={"rep": xpart}, device_id_type=MESH)
    pl.semaphore_wait(bar, F + 3)

    def source(k, tt):
        return g_refs[k // split].at[tt, :, pl.ds((k % split) * rows, rows)]

    def load(k, j):
        return pltpu.make_async_copy(source(k, t if j == 0 else ypart), acc.at[k, j], lsem.at[k, j])

    def c_copy(k, j):
        return rc(source(k, core if j == 0 else core ^ 2), cin.at[k, j], cs.at[k, j], cr.at[k, j], tensor=core)

    def x_copy(k):
        return rc(acc.at[k, 1, :, other], xin.at[k], xs.at[k], xr.at[k], rep=xpart)

    def y_copy(k):
        return rc(acc.at[k, 1, :, mine], yin.at[k], ys.at[k], yr.at[k], tensor=ypart)

    def z_copy(k, dst, down):
        buf = zdn if down else zup
        return rc(acc.at[k, 0, dst], buf.at[k, dst], zs.at[k, dst], zr.at[k, dst, 0 if down else 1],
                  frame=f - 1 if down else f + 1)

    def pair_copy():
        return rc(h_ref, hin, hs, hr, rep=xpart)

    def fin_copy(k):
        return rc(acc.at[k, 0, f], fin.at[k], fs.at[k], fr_.at[k], rep=xpart)

    def small_copy(i):
        if i == 0:
            return rc(s_ref.at[pl.ds(0, 2), 1 - t % 2], scin, ss.at[0], sr.at[0], tensor=core)
        if i == 1:
            return rc(sacc, sxin, ss.at[1], sr.at[1], rep=xpart)
        return rc(sacc.at[1 - t // 2], syin, ss.at[2], sr.at[2], tensor=ypart)

    def small_frames(fn):
        for d in range(1, F):
            for to in (f - d, f + d):
                @pl.when((to >= 0) & (to < F))
                def _():
                    fn(to)

    def small_step(i):
        if 0 < i < 4:
            small_copy(i - 1).wait()
        if i == 1:
            for yy in range(2):
                sacc[yy] = s_ref[yy, t % 2] + scin[yy]
        elif i == 2:
            sacc[...] += sxin[...]
        elif i == 3:
            syin[...] += sacc[t // 2]
            small_frames(lambda to: rc(syin.at[to], szin.at[f], ss.at[3 + to], sr.at[3 + f], frame=to).start())
        elif i == 4:
            small_frames(lambda to: rc(syin.at[to], szin.at[to], ss.at[3 + to], sr.at[3 + to], frame=to).wait())
            szin[f] = syin[f]
            out = szin[0]
            for n in range(1, F):
                out = out + szin[n]
            sout_ref[...] = out
        if i < 3:
            small_copy(i).start()

    for k in range(K):
        for j in (1, 0):
            c_copy(k, j).start()
            load(k, j).start()

    def add(k, j):
        c_copy(k, j).wait_recv()
        load(k, j).wait()
        @pl.loop(0, F)
        def _(i):
            acc[k, j, i] = acc[k, j, i] + cin[k, j, i]

    def step_a(k):
        add(k, 1)
        x_copy(k).start()
        add(k, 0)

    def step_b(k):
        x_copy(k).wait()
        @pl.loop(0, F)
        def _(i):
            acc[k, 1, i, mine] = acc[k, 1, i, mine] + xin[k, i]
        y_copy(k).start()

    def step_c(k):
        y_copy(k).wait()
        @pl.loop(0, F)
        def _(i):
            acc[k, 0, i, mine] = acc[k, 0, i, mine] + yin[k, i]
        for dst in range(F):
            @pl.when((f == F - 1) & (dst < f))
            def _():
                z_copy(k, dst, True).start()
            up = F - 1 - dst
            @pl.when((f == 0) & (up > f))
            def _():
                z_copy(k, up, False).start()

    def take(k, dst, down):
        buf = zdn if down else zup
        rc(buf.at[k, dst], buf.at[k, dst], zs.at[k, dst], zr.at[k, dst, 0 if down else 1], frame=f).wait_recv()
        acc[k, 0, dst] = acc[k, 0, dst] + buf[k, dst]
        @pl.when(dst != f)
        def _():
            z_copy(k, dst, down).start()

    def step_d(k):
        for hop in range(1, F):
            @pl.when(f == F - 1 - hop)
            def _():
                lax.fori_loop(0, F - hop, lambda dst, c: take(k, dst, True) or c, 0)
            @pl.when(f == hop)
            def _():
                lax.fori_loop(0, F - hop, lambda i, c: take(k, F - 1 - i, False) or c, 0)
        fin_copy(k).start()

    def step_e(k):
        fin_copy(k).wait()
        part = pl.ds((k % split) * rows, rows)
        out_ref[k // split, part, :] = acc[k, 0, f].astype(F32) + fin[k].astype(F32)

    steps = (step_a, step_b, step_c, step_d, step_e)
    for s in range(K + len(steps) - 1):
        for i, fn in enumerate(steps):
            if 0 <= s - i < K:
                fn(s - i)
        if s < 5:
            small_step(s)
        if s == 1:
            rows_start(T, t, rc, (a_ref,), (ao_ref,), False, rs, rr, rl)
        if s == K - 1:
            pair_copy().start()
    pair_copy().wait()
    for i in range(h_ref.shape[0]):
        out_ref[G + i] = h_ref[i].astype(F32) + hin[i].astype(F32)
    rows_wait(T, t, rc, (a_ref,), (ao_ref,), False, rs, rr, rl)
    for k in range(K):
        for j in (1, 0):
            c_copy(k, j).wait_send()
        for dst in range(F):
            @pl.when(dst < f)
            def _():
                z_copy(k, dst, True).wait_send()
            @pl.when(dst > f)
            def _():
                z_copy(k, dst, False).wait_send()


def reduce_all(grads, half, small, a):
    F, T = lax.axis_size("frame"), lax.axis_size("tensor")
    G = len(grads)
    K = G * SPLIT
    _, _, full, D = grads[0].shape
    rows = full // SPLIT
    dma = pltpu.SemaphoreType.DMA
    V = pltpu.VMEM
    sm = small.shape[2:]
    sds = jax.ShapeDtypeStruct
    any_spec, vmem = pl.BlockSpec(memory_space=pl.ANY), pl.BlockSpec(memory_space=pltpu.VMEM)
    split_rows = (a.shape[1], a.shape[0]) + a.shape[2:]
    return pl.pallas_call(
        partial(reduce_kernel, F, T, G, SPLIT),
        out_shape=(sds((G + half.shape[0], full, D), F32), sds(sm, F32), sds(split_rows, a.dtype)),
        in_specs=[any_spec] * G + [vmem] * 3,
        out_specs=(vmem, vmem, any_spec),
        scratch_shapes=[
            V((K, 2, F, rows, D), BF), V((K, 2, F, rows, D), BF), V((K, F, rows // 2, D), BF), V((K, F, rows // 2, D), BF),
            V((K, F, rows, D), BF), V((K, F, rows, D), BF), V((K, rows, D), BF),
            V((2, F) + sm, F32), V((2, F) + sm, F32), V((2, F) + sm, F32), V((F,) + sm, F32), V((F,) + sm, F32),
            dma((K, 2)), dma((K, 2)), dma((K, 2)), dma((K,)), dma((K,)), dma((K,)), dma((K,)),
            dma((K, F)), dma((K, F, 2)), dma((K,)), dma((K,)), dma((3 + F,)), dma((3 + F,)),
            dma((1, T)), dma((1, T)), dma((1,)), V(half.shape, BF), dma(()), dma(()),
        ],
        compiler_params=pltpu.CompilerParams(collective_id=1, has_side_effects=True, vmem_limit_bytes=62 * 1024 * 1024),
        name="reduce_all",
    )(*grads, half, small.reshape((2, T // 2, F) + sm).astype(F32), a)


def remote(src, dst, ssem, rsem, **dev):
    return pltpu.make_async_remote_copy(src, dst, ssem, rsem, device_id=dev, device_id_type=MESH)


def others(F, f, fn):
    for d in range(F - 1, 0, -1):
        for to in (f - d, f + d):
            pl.when((to >= 0) & (to < F))(partial(fn, to))


def greet(F, T, f, t, cores):
    bar = pltpu.get_barrier_semaphore()

    def signal(to, tt):
        pl.semaphore_signal(bar, inc=1, device_id={"frame": to, "tensor": tt}, device_id_type=MESH)

    for j in range(cores):
        others(F, f, lambda to: signal(to, t ^ j))
    for p in range(1, T):
        signal(f, t ^ p)
    pl.semaphore_wait(bar, cores * (F - 1) + T - 1)


def rows_to_both(F, T, s_ref, a_ref, o_ref, ao_ref, zs, zr, cs, cr, ls, rs, rr, rl):
    f, t = lax.axis_index("frame"), lax.axis_index("tensor")
    greet(F, T, f, t, 1)

    def z_copy(to, frm):
        return remote(s_ref.at[:, to], o_ref.at[0, frm], zs.at[to], zr.at[frm], frame=to)

    def c_copy(frm):
        return remote(o_ref.at[0, frm], o_ref.at[1, frm], cs.at[frm], cr.at[frm], tensor=t ^ 1)

    others(F, f, lambda to: z_copy(to, f).start())
    rows_start(T, t, remote, (a_ref,), (ao_ref,), True, rs, rr, rl)
    own = remote(s_ref.at[:, f], o_ref.at[1, f], cs.at[f], cr.at[f], tensor=t ^ 1)
    own.start()
    local = pltpu.make_async_copy(s_ref.at[:, f], o_ref.at[0, f], ls)
    local.start()

    def arrive(frm):
        z_copy(frm, frm).wait_recv()
        c_copy(frm).start()

    others(F, f, arrive)

    def finish(frm):
        z_copy(frm, f).wait_send()
        c_copy(frm).wait_send()
        c_copy(frm).wait_recv()

    others(F, f, finish)
    rows_wait(T, t, remote, (a_ref,), (ao_ref,), True, rs, rr, rl)
    own.wait()
    local.wait()


def cross(F, T, to_frames, *refs):
    if to_frames:
        s_ref, o_ref, ss, sr, ls = refs
    else:
        s_ref, a_ref, o_ref, ao_ref, ss, sr, ls, *row_sems = refs
    f, t = lax.axis_index("frame"), lax.axis_index("tensor")
    greet(F, T, f, t, 2)

    def src(j, to):
        return s_ref.at[j, to] if to_frames else s_ref.at[j, :, to]

    def dst(j, frm):
        return o_ref.at[j, :, frm] if to_frames else o_ref.at[j, frm]

    def copy(j, to, frm):
        return remote(src(j, to), dst(j, frm), ss.at[j, to], sr.at[j, frm], frame=to, tensor=t ^ j)

    for j in (1, 0):
        others(F, f, lambda to: copy(j, to, f).start())
    copy(1, f, f).start()
    if not to_frames:
        rows_start(T, t, remote, (a_ref,), (ao_ref,), False, *row_sems)
    local = pltpu.make_async_copy(src(0, f), dst(0, f), ls)
    local.start()

    def finish(j, frm):
        copy(j, frm, f).wait_send()
        copy(j, frm, frm).wait_recv()

    for j in (1, 0):
        others(F, f, partial(finish, j))
    if not to_frames:
        rows_wait(T, t, remote, (a_ref,), (ao_ref,), False, *row_sems)
    copy(1, f, f).wait()
    local.wait()


def sum_to_frames(F, T, a_ref, b_ref, o_ref, cin, buf, cs, cr, zs, zr, ls):
    f, t = lax.axis_index("frame"), lax.axis_index("tensor")
    greet(F, T, f, t, 1)

    def c_copy(to):
        return remote(b_ref.at[to], cin.at[to], cs.at[to], cr.at[to], tensor=t ^ 1)

    def z_copy(to, frm):
        return remote(buf.at[to], o_ref.at[:, frm], zs.at[to], zr.at[frm], frame=to)

    def add(to):
        c_copy(to).wait_recv()
        @pl.loop(0, buf.shape[1])
        def _(i):
            buf[to, i] = (a_ref[to, i] + cin[to, i].astype(F32)).astype(BF)

    def send(to):
        add(to)
        z_copy(to, f).start()

    others(F, f, lambda to: c_copy(to).start())
    c_copy(f).start()
    others(F, f, send)
    add(f)
    local = pltpu.make_async_copy(buf.at[f], o_ref.at[:, f], ls)
    local.start()

    def finish(frm):
        c_copy(frm).wait_send()
        z_copy(frm, f).wait_send()
        z_copy(frm, frm).wait_recv()

    others(F, f, finish)
    c_copy(f).wait_send()
    local.wait()


def exchange(body, ins, out_shapes, scratch, collective_id, name):
    return pl.pallas_call(
        body,
        out_shape=tuple(jax.ShapeDtypeStruct(s, BF) for s in out_shapes),
        in_specs=[pl.BlockSpec(memory_space=pltpu.VMEM)] * len(ins),
        out_specs=(pl.BlockSpec(memory_space=pltpu.HBM),) * len(out_shapes),
        scratch_shapes=scratch,
        compiler_params=pltpu.CompilerParams(
            collective_id=collective_id, has_side_effects=True, vmem_limit_bytes=62 * 1024 * 1024
        ),
        name=name,
    )(*ins)


def shards(
    tokens, query_space, key_space, value_space, output_space, query_time, key_time, value_time,
    output_time, mlp_in, bias_in, mlp_out, bias_out, gain_first, shift_first, gain_second,
    shift_second, gain_third, shift_third, place_slot, cotangent,
):
    F = lax.axis_size("frame")
    T = lax.axis_size("tensor")
    clips, frames_dev, places_dev, D = tokens.shape
    width = query_space.shape[1]
    heads = width // HEAD
    hid = mlp_in.shape[1]
    rows_w = query_space.shape[0]
    fr = clips * frames_dev // T
    fp = frames_dev // fr
    R = fr * T * PAD
    f_id = lax.axis_index("frame")
    t_id = lax.axis_index("tensor")
    core = t_id % 2

    def pack(q, k, v, o):
        return jnp.concatenate((q, k, v, o.T), axis=1)

    wl = jnp.stack(
        (
            pack(query_space, key_space, value_space, output_space),
            pack(query_time, key_time, value_time, output_time),
        )
    )
    part_bin = lax.dynamic_slice(bias_in, (f_id * (hid // F),), (hid // F,)).astype(F32)
    part_bout = lax.dynamic_slice(
        bias_out, (t_id * (bias_out.shape[0] // T),), (bias_out.shape[0] // T,)
    ).astype(F32)
    small = jnp.concatenate(
        (gain_first, shift_first, gain_second, shift_second, gain_third, shift_third, part_bout, part_bin)
    )

    def lanes(flat):
        pad = -flat.shape[-1] % 1024
        flat = jnp.pad(flat, [(0, 0)] * (flat.ndim - 1) + [(0, pad)])
        return flat.reshape(flat.shape[:-1] + (-1, 128))

    def split_places(v):
        v = jnp.pad(v, ((0, 0), (0, 0), (0, PAD - places_dev), (0, 0)))
        return v.reshape(T, fr, PAD, D)

    W, small_all, x = gather_all(wl, lanes(small), split_places(tokens))
    FT = ("frame", "tensor")
    W, wl_mlp = lax.optimization_barrier((W, jnp.stack((mlp_in, mlp_out.T))))
    W_mlp = lax.all_gather(wl_mlp, FT, axis=0, tiled=False).reshape(F, T, 2, rows_w, D)
    W = W.reshape(2, T, F * rows_w, D)
    x = x.reshape(R, D)
    small_all = small_all.reshape(T, F, -1)
    nv = 7 * gain_first.shape[0]
    vec = small_all[:, :, :nv].reshape(T, F, 7, -1).transpose(2, 1, 0, 3).reshape(7, D)
    vec = jnp.concatenate((vec, jnp.zeros((1, D), F32)), axis=0)
    bin_all = small_all[:, :, nv : nv + hid // F].reshape(T, hid)

    keep = place_slot >= 0
    bias = jnp.where(keep, 0.0, -1e30).astype(F32).reshape(T, places_dev)
    bias = jnp.pad(bias, ((0, 0), (0, PAD - places_dev)), constant_values=-1e30).reshape(1, T * PAD)
    rows = T * PAD

    qkv_s, os_s, xs, ht = call(
        partial(space_forward, width, heads, fr, rows),
        T,
        (x, vec, bias, W),
        [whole((R, D)), whole((8, D)), whole((1, rows)), pl.BlockSpec((1, 1, D, D), lambda t: (0, t, 0, 0))],
        [((T, R, 3 * width), BF), ((T, R, width), BF), ((R, D), F32), ((R, D), BF)],
        [
            pl.BlockSpec((1, R, 3 * width), lambda t: (t, 0, 0)),
            pl.BlockSpec((1, R, width), lambda t: (t, 0, 0)),
            whole((R, D)),
            whole((R, D)),
        ],
        [pltpu.VMEM((R, D), BF)],
        name="space_forward",
    )

    groups = PAD // 8
    nf = 2 * F * fr
    size = nf * 8
    RT = groups * size

    def group_rows(a, b):
        v = jnp.stack((a, b)).reshape(nf, groups, 8, a.shape[-1])
        return v.transpose(1, 0, 2, 3).reshape(RT, a.shape[-1])

    def ungroup_rows(v):
        n = v.shape[-1]
        return v.reshape(groups, nf, 8, n).transpose(1, 0, 2, 3).reshape(2, F, fr, PAD, n)

    dma = pltpu.SemaphoreType.DMA
    row_sems = [dma((1, T)), dma((1, T)), dma((1,))]
    h_both, cot = exchange(
        partial(rows_to_both, F, T),
        (ht.reshape(fr, F, PAD, D), split_places(cotangent)),
        ((2, F, fr, PAD, D), (fr, T, PAD, D)),
        [dma((F,)), dma((F,)), dma((F,)), dma((F,)), dma(())] + row_sems,
        2,
        "rows_to_both",
    )
    cot = cot.reshape(R, D)
    h_t = group_rows(h_both[0], h_both[1])
    keep_q = lax.dynamic_slice(
        jnp.pad(keep.astype(F32).reshape(T, places_dev), ((0, 0), (0, PAD - places_dev))), (f_id, 0), (1, PAD)
    )
    mask = jnp.broadcast_to(keep_q.reshape(groups, 1, 8), (groups, nf, 8)).reshape(RT, 1)
    core_arr = core.reshape(1).astype(jnp.int32)
    halves = T // 2
    time_w = pl.BlockSpec((1, 1, D, D), lambda i, c: (1, c[0] + 2 * i, 0, 0))
    per_half = lambda n: pl.BlockSpec((1, RT, n), lambda i, c: (i, 0, 0))
    qkv_t, ot = call(
        partial(time_forward, width, heads, groups, size, 8),
        halves,
        (core_arr, h_t, W, mask),
        [whole((RT, D)), time_w, whole((RT, 1))],
        [((halves, RT, 3 * width), BF), ((halves, RT, width), BF)],
        [per_half(3 * width), per_half(width)],
        [],
        prefetch=1,
        name="time_forward",
    )
    ot_u = jnp.stack([ungroup_rows(ot[i]) for i in range(halves)], axis=-2)
    ot_u = ot_u.reshape(2, F, fr, PAD, halves * width)
    cross_sems = [dma((2, F)), dma((2, F)), dma(())]
    (ot_both,) = exchange(
        partial(cross, F, T, True), (ot_u,), ((2, fr, F, PAD, halves * width),), cross_sems, 3, "ot_to_frames"
    )
    win_spec = lambda kind: pl.BlockSpec((F, 1, 1, rows_w, D), lambda t, c: (0, t, kind, 0, 0))
    res, gt, dot_both, g_mlp, g_wt, sv_m, gb = call(
        partial(mlp_both, width, halves),
        T,
        (core_arr, xs, cot, ot_both.reshape(2, R, halves * width), vec, bin_all, W, W_mlp, W_mlp),
        [
            whole((R, D)), whole((R, D)), whole((2, R, halves * width)), whole((8, D)), whole((T, hid)),
            pl.BlockSpec((1, T, D, D), lambda t, c: (1, 0, 0, 0)), win_spec(0), win_spec(1),
        ],
        [
            ((R, D), BF), ((R, D), F32), ((2, R, halves * width), BF), ((F, T, 2, rows_w, D), BF),
            ((T, D, width), BF), ((8, D), F32), ((T, hid), F32),
        ],
        [
            whole((R, D)), whole((R, D)), whole((2, R, halves * width)),
            pl.BlockSpec((F, 1, 2, rows_w, D), lambda t, c: (0, t, 0, 0, 0)),
            whole((T, D, width)), whole((8, D)), whole((T, hid)),
        ],
        [pltpu.VMEM((R, D), F32), pltpu.VMEM((R, D), BF), pltpu.VMEM((R, D), F32), pltpu.VMEM((R, D), F32)],
        prefetch=1,
        name="mlp_both",
    )
    share_mlp = lax.psum_scatter(
        g_mlp.reshape(F * T, 2, rows_w, D), FT, scatter_dimension=0, tiled=False
    )
    d_both, res_rows = exchange(
        partial(cross, F, T, False),
        (dot_both.reshape(2, fr, F, PAD, halves * width), res.reshape(fr, T, PAD, D)),
        ((2, F, fr, PAD, halves * width), (T, fr, PAD, D)),
        cross_sems + row_sems,
        4,
        "dot_to_time",
    )
    d_t = group_rows(d_both[0], d_both[1]).reshape(RT, halves, width).transpose(1, 0, 2)
    g_time, dh_part = call(
        partial(time_backward, width, heads, groups, size, 8),
        T,
        (core_arr, h_t, W, mask, qkv_t, d_t, g_wt),
        [
            whole((RT, D)), pl.BlockSpec((1, 1, D, D), lambda t, c: (1, c[0] + 2 * (t // 2), 0, 0)), whole((RT, 1)),
            pl.BlockSpec((1, RT, 3 * width), lambda t, c: (t // 2, 0, 0)),
            pl.BlockSpec((1, RT, width), lambda t, c: (t // 2, 0, 0)),
            pl.BlockSpec((1, D, width), lambda t, c: (t, 0, 0)),
        ],
        [((T, D, D), BF), ((RT, D), F32)],
        [pl.BlockSpec((1, D, D), lambda t, c: (t, 0, 0)), whole((RT, D))],
        [pltpu.VMEM((RT, 3 * width), BF)],
        prefetch=1,
        name="time_backward",
    )
    dh_u = ungroup_rows(dh_part)
    (dht,) = exchange(
        partial(sum_to_frames, F, T),
        (dh_u[0], dh_u[1].astype(BF)),
        ((fr, F, PAD, D),),
        [pltpu.VMEM((F, fr, PAD, D), BF)] * 2 + [dma((F,)), dma((F,)), dma((F,)), dma((F,)), dma(())],
        5,
        "sum_to_frames",
    )
    dht = dht.reshape(R, D)

    gx, g_space, sv_s = call(
        partial(space_backward, width, heads, fr, rows),
        T,
        (x, xs, gt, dht, vec, bias, W, qkv_s, os_s),
        [
            whole((R, D)), whole((R, D)), whole((R, D)), whole((R, D)), whole((8, D)), whole((1, rows)),
            pl.BlockSpec((1, 1, D, D), lambda t: (0, t, 0, 0)),
            pl.BlockSpec((1, R, 3 * width), lambda t: (t, 0, 0)),
            pl.BlockSpec((1, R, width), lambda t: (t, 0, 0)),
        ],
        [((R, D), BF), ((T, D, D), BF), ((8, D), F32)],
        [whole((R, D)), pl.BlockSpec((1, D, D), lambda t: (t, 0, 0)), whole((8, D))],
        [
            pltpu.VMEM((R, D), BF), pltpu.VMEM((R, D), F32), pltpu.VMEM((R, D), BF), pltpu.VMEM((R, D), F32),
            pltpu.VMEM((R, 3 * width), BF), pltpu.VMEM((R, width), BF),
        ],
        name="space_backward",
    )
    kinds = tuple(g.reshape(T, F, rows_w, D) for g in (g_space, g_time))
    n = gain_first.shape[0]
    nb = bias_out.shape[0]
    norms = jnp.concatenate((sv_s[0:4], sv_m[0:2]), axis=0).reshape(6, F, T, n).transpose(2, 1, 0, 3)
    small_g = jnp.concatenate(
        (
            norms.reshape(T, F, 6 * n),
            jnp.broadcast_to(sv_m[2].reshape(1, F, nb), (T, F, nb)),
            jnp.broadcast_to(gb[:, None, :], (T, F, hid)),
        ),
        axis=2,
    )
    share, smalls, gx_rows = reduce_all(kinds, share_mlp, lanes(small_g), gx.reshape(fr, T, PAD, D))
    reps = lax.axis_size("rep")
    if reps > 2:
        share, smalls = (lax.psum(0.5 * v, "rep") for v in (share, smalls))
    smalls = smalls.reshape(-1)

    def join_places(v):
        return v.reshape(clips, frames_dev, PAD, D)[:, :, :places_dev]

    def unpack(g):
        return g[:, :width], g[:, width : 2 * width], g[:, 2 * width : 3 * width], g[:, 3 * width :].T

    gs_q, gs_k, gs_v, gs_o = unpack(share[0])
    gt_q, gt_k, gt_v, gt_o = unpack(share[1])
    own = lambda i: smalls[i * n : (i + 1) * n]
    return (
        join_places(res_rows),
        join_places(gx_rows).astype(F32),
        gs_q, gs_k, gs_v, gs_o,
        gt_q, gt_k, gt_v, gt_o,
        share[2],
        smalls[6 * n + nb : 6 * n + nb + hid],
        share[3].T,
        smalls[6 * n : 6 * n + nb],
        own(0), own(1), own(2), own(3), own(4), own(5),
    )


def solution(mesh):
    rows = P("rep", "frame", "tensor", None)
    ft, tf, vec = P("frame", "tensor"), P("tensor", "frame"), P(("frame", "tensor"))
    placed = (
        rows, ft, ft, ft, tf, ft, ft, ft, tf, ft, P("tensor"), tf, P("frame"),
        vec, vec, vec, vec, vec, vec, P(), rows,
    )
    return jax.shard_map(
        shards,
        mesh=mesh,
        in_specs=placed,
        out_specs=(
            rows, rows, ft, ft, ft, tf, ft, ft, ft, tf, ft, P("tensor"), tf, P("frame"),
            vec, vec, vec, vec, vec, vec,
        ),
        check_vma=False,
    )
```
